32 devices in a mesh: dp: 4 (over y, x), expert: 8 (over z, core).
Axes of the slice: x: 2, y: 2, z: 4, core: 2. Of those that a mesh axis runs over, the one named last changes fastest.
Arguments:
- tokens: bfloat16 [4096, 2048], P(('dp', 'expert')), may hold values from -6 to 6
- teacher: bfloat16 [4096, 2048], P(('dp', 'expert')), may hold values from -6 to 6
- qkv_weight: bfloat16 [2048, 6144], P('dp'), may hold values from -0.125 to 0.125
- out_weight: bfloat16 [2048, 2048], P('dp'), may hold values from -1 to 1
- query_gain: float32 [128], replicated, may hold values from 0.5 to 1.5
- key_gain: float32 [128], replicated, may hold values from 0.5 to 1.5
- attn_gain: float32 [2048], replicated, may hold values from 0.5 to 1.5
- ffn_gain: float32 [2048], replicated, may hold values from 0.5 to 1.5
- router_weight: bfloat16 [2048, 16], replicated, may hold values from -0.0625 to 0.0625
- gate_up_weight: bfloat16 [16, 2048, 2048], P('expert', 'dp'), may hold values from -0.125 to 0.125
- down_weight: bfloat16 [16, 1024, 2048], P('expert', 'dp'), may hold values from -1.5 to 1.5
- deal: int32 [32], replicated, may hold values from 0 to 31, each once
- routes: int32 [4096, 8], P(('dp', 'expert')), may hold values from 0 to 15, all different within a row; in each aligned block of 128 rows (0 to 127, 128 to 255, ...) at most 128 rows name the same one
- counted: int32 [4096], P(('dp', 'expert')), may hold values from 0 to 1, as said below
- lengths: int32 [32, 4], P(('dp', 'expert')), may hold values from 1 to 64, 128 in all within a row
Outputs:
- output: bfloat16 [4096, 2048], P(('dp', 'expert'))
- mean_loss: float32 [], replicated
- d_tokens: float32 [4096, 2048], P(('dp', 'expert'))
- d_qkv_weight: float32 [2048, 6144], P(('dp', 'expert'))
- d_out_weight: float32 [2048, 2048], P(('dp', 'expert'))
- d_query_gain: float32 [128], replicated
- d_key_gain: float32 [128], replicated
- d_attn_gain: float32 [2048], replicated
- d_ffn_gain: float32 [2048], replicated
- d_router_weight: float32 [2048, 16], replicated
- d_gate_up_weight: float32 [16, 2048, 2048], P('expert', 'dp')
- d_down_weight: float32 [16, 1024, 2048], P('expert', 'dp')
The draws below stay inside these ranges and needn't reach their ends.
Inputs may be any that keep to these rules, and one draw needn't show every extreme that they name: `routes`: each row names 8 different experts; among the 128 dealt rows of one device no expert is named more than 128 times, and in every draw some expert is named exactly 128 times on some device. Row d holds the lengths of the sequences that fill the block dealt to device d, in order; each row sums to 128 and its largest entry is exactly 64. `counted`: 1 marks a token whose error enters the loss. `deal`: each block number appears once.
All inputs are finite; a program needn't handle non-finite values.
Results may differ from the reference program's by a relative error of at most 0.017.
Values may be sent and summed in bfloat16 or wider, within the bound.
A program may use at most 320 MiB of HBM per device.

```python
import math
import jax
import jax.numpy as jnp
import numpy as np
from jax import lax

D = 2048
H = 16
HD = 128
FFE = 1024
TOPK = 8
SEQ_DEV = 4
TOK_DEV = 128
TOKENS = 4096
STRIPE = 4
EXPERTS = 16
CAP = 128
SEQ_MAX = 64
DEVICES = 32


def draw_counted(key, part):
    tok_index = jnp.arange(TOKENS, dtype=jnp.int32)
    block_index = tok_index // TOK_DEV
    threshold = 250 + 500 * block_index // max(DEVICES - 1, 1)
    ticket = jax.random.randint(key, (TOKENS,), 0, 1000, dtype=jnp.int32)
    return (ticket < threshold).astype(jnp.int32)


def shard_levels(key, extent, cuts, low, top_value):
    def one(axis_at, shards_of):
        draws = jax.random.uniform(jax.random.fold_in(jax.random.fold_in(key, 6), axis_at), (shards_of,), jnp.float32, low / len(cuts), top_value / len(cuts))
        return jnp.repeat(jnp.exp(draws), extent[axis_at] // shards_of).reshape((-1,) + (1,) * (len(extent) - axis_at - 1))

    gain = one(*cuts[0])
    for cut in cuts[1:]:
        gain = gain * one(*cut)
    return gain


def profile(count, total, reach, slope):
    loads = [(1 << 20) // math.isqrt(grade ** slope) + 1 for grade in range(2, count + 1)]
    surplus, counts = total - reach - (count - 1), [1] * (count - 1)
    while surplus > 0:
        movable = [i for i in range(count - 1) if counts[i] < reach]
        mass, remaining = sum([loads[i] for i in movable]), surplus
        for i in movable:
            addition = min(reach - counts[i], max(1, remaining * loads[i] // mass), surplus)
            counts[i] = counts[i] + addition
            surplus = surplus - addition
    return np.array([reach] + counts)


def uneven_parts(key, count, total, most, slope):
    if count == 2:
        one = jax.random.randint(key, (), max(1, total - most), min(most, total - 1) + 1)
        return jnp.stack([one, total - one])
    tallies = jnp.asarray(profile(count, total, most, slope), jnp.int32)
    twos = (count - 1) // 2
    giver, receiver = tallies[1:1 + 2 * twos:2], tallies[2:2 + 2 * twos:2]
    margin = jnp.minimum(giver - 1, most - receiver)
    moved = jax.random.randint(jax.random.fold_in(key, 1), (twos,), 0, 1 << 20) % (margin + 1)
    tallies = tallies.at[1:1 + 2 * twos:2].set(giver - moved).at[2:2 + 2 * twos:2].set(receiver + moved)
    return tallies[jax.random.permutation(jax.random.fold_in(key, 2), count)]


def assign_block(rng, own, number, rows, number_of, top, reach, lean):
    order = jax.random.permutation(rng, number_of)
    crowded, common = portions_of(number_of, rows * top, reach, lean, True), portions_of(number_of, rows * top, reach, lean, False)
    places = jnp.arange(number_of)

    def named(sizes, turn):
        used = int((sizes > 0).sum())
        fixed = max(1, used // 4)
        shifted = fixed + (places - fixed + turn * (used - fixed)) % max(1, number_of - fixed)
        return jnp.zeros((number_of,), jnp.int32).at[order[jnp.where(places < fixed, places, shifted)]].set(jnp.asarray(sizes, jnp.int32))

    sizes = jnp.where(number % 4 == 0, named(crowded, number // 4), named(common, number - number // 4 - 1))
    mixed = jax.random.permutation(jax.random.fold_in(own, 3), number_of)
    giver, sink = mixed[0:number_of // 2 * 2:2], mixed[1:number_of // 2 * 2:2]
    margin = jnp.minimum(sizes[giver] - 1, reach - sizes[sink]) // 2
    margin = jnp.where((giver == order[0]) | (sink == order[0]) | (sizes[sink] == 0), 0, jnp.maximum(margin, 0))
    shifted = jax.random.randint(jax.random.fold_in(own, 4), (number_of // 2,), 0, 1 << 20) % (margin + 1)
    sizes = sizes.at[giver].add(-shifted).at[sink].add(shifted)
    labels = jnp.searchsorted(jnp.cumsum(sizes), jnp.arange(rows * top), side="right").astype(jnp.int32)
    grid = labels.reshape(top, rows).T
    grid = grid[jax.random.permutation(jax.random.fold_in(own, 1), rows)]
    turn = jax.random.randint(jax.random.fold_in(own, 2), (rows, 1), 0, top)
    return jnp.take_along_axis(grid, (jnp.arange(top)[None, :] + turn) % top, axis=1)


def portions_of(amount, total, reach, lean, full):
    portions = [(1 << 20) // math.isqrt(grade ** lean) + 1 for grade in range(1, amount + 1)]
    largest = reach if full else min(reach, max(-(-total // amount), total * portions[0] // sum(portions)))
    least = 1 if total - largest >= amount - 1 else 0
    holding, rest = [largest] + [least] * (amount - 1), total - largest - least * (amount - 1)
    while rest > 0:
        movable = [i for i in range(1, amount) if holding[i] < largest] or [i for i in range(1, amount) if holding[i] < reach]
        mass, remaining = sum([portions[i] for i in movable]), rest
        for i in movable:
            more = min(reach - holding[i], max(1, remaining * portions[i] // mass), rest)
            holding[i] = holding[i] + more
            rest = rest - more
    return np.array(holding)


def scatter_about(own_key, extent, deviation, limit, shards=(), held_as=jnp.bfloat16):
    gain = shard_levels(own_key, extent, shards, -0.22, 0.18) if shards else 1.0
    drawn = jax.random.normal(own_key, extent, jnp.float32) * deviation * gain
    return jnp.minimum(jnp.maximum(drawn, -limit), limit).astype(held_as)


def setup_inputs(seed: int = 0) -> dict:
    splits = jax.random.split(jax.random.key(seed), 16)
    tokens = scatter_about(splits[0], (TOKENS, D), 1.0, 6.0, ((0, 32),))
    teacher = scatter_about(splits[1], (TOKENS, D), 1.0, 6.0, ((0, 32),))
    qkv_weight = scatter_about(splits[2], (D, 3 * D), D ** -0.5, 0.125, ((0, 4),))
    out_weight = scatter_about(splits[3], (D, D), (D // 64) ** -0.5, 1.0, ((0, 4),))
    query_gain = jnp.clip(1.0 + 0.1 * jax.random.normal(splits[4], (HD,), jnp.float32), 0.5, 1.5)
    key_gain = jnp.clip(1.0 + 0.1 * jax.random.normal(splits[5], (HD,), jnp.float32), 0.5, 1.5)
    attn_gain = jnp.clip(1.0 + 0.1 * jax.random.normal(splits[6], (D,), jnp.float32), 0.5, 1.5)
    ffn_gain = jnp.clip(1.0 + 0.1 * jax.random.normal(splits[7], (D,), jnp.float32), 0.5, 1.5)
    router_weight = scatter_about(splits[8], (D, EXPERTS), (4 * D) ** -0.5, 0.0625)
    gate_up_weight = scatter_about(splits[9], (EXPERTS, D, 2 * FFE), D ** -0.5, 0.125, ((0, 8), (1, 4)))
    down_weight = scatter_about(splits[10], (EXPERTS, FFE, D), (FFE // 64) ** -0.5, 1.5, ((0, 8), (1, 4)))
    deal = jax.random.permutation(splits[11], DEVICES).astype(jnp.int32)
    routes_keys = jax.random.split(jax.random.fold_in(splits[12], 1), TOKENS // TOK_DEV)
    routes_turns = jax.random.permutation(jax.random.fold_in(splits[12], 3), TOKENS // TOK_DEV)
    routes = jax.vmap(lambda own, number: assign_block(jax.random.fold_in(splits[12], 2), own, number, TOK_DEV, EXPERTS, TOPK, CAP, 1))(routes_keys, routes_turns).reshape((TOKENS, TOPK))
    counted = draw_counted(jax.random.fold_in(splits[15], 71), 0)
    lengths = jax.vmap(lambda own: uneven_parts(own, SEQ_DEV, TOK_DEV, SEQ_MAX, 2))(jax.random.split(splits[14], DEVICES)).reshape((DEVICES, SEQ_DEV)).astype(jnp.int32)
    return dict(tokens=tokens, teacher=teacher, qkv_weight=qkv_weight, out_weight=out_weight, query_gain=query_gain, key_gain=key_gain, attn_gain=attn_gain, ffn_gain=ffn_gain, router_weight=router_weight, gate_up_weight=gate_up_weight, down_weight=down_weight, deal=deal, routes=routes, counted=counted, lengths=lengths)


@jax.custom_vjp
def low(v):
    return lax.optimization_barrier(v.astype(jnp.bfloat16)).astype(jnp.float32)

@jax.custom_vjp
def low_back(v):
    return v

def low_keep(v):
    return (low(v), None)

def low_pass(kept, grad):
    return (grad,)

def back_keep(v):
    return (v, None)

def back_low(kept, grad):
    return (low(grad),)
low.defvjp(low_keep, low_pass)
low_back.defvjp(back_keep, back_low)
EPS = 1e-06
ROPE_BASE = 50000.0

def exact_dot(left, right):
    return jnp.dot(left, right, precision=lax.Precision.HIGHEST, preferred_element_type=jnp.float32)

def rms_scale(values):
    return lax.rsqrt(lax.optimization_barrier(jnp.mean(values * values, axis=-1, keepdims=True)) + EPS)

def rotate(values, cosine, sine_part):
    half_size = values.shape[-1] // 2
    first_half = values[..., :half_size]
    second_half = values[..., half_size:]
    return jnp.concatenate([first_half * cosine - second_half * sine_part, second_half * cosine + first_half * sine_part], axis=-1)

def deal_order(given, deal):
    width = given.shape[-1]
    blocks = given.reshape(DEVICES, DEVICES, STRIPE, width).transpose(1, 0, 2, 3).reshape(DEVICES, TOK_DEV, width)
    return blocks[deal].reshape(TOKENS, width)

def given_order(dealt, deal):
    width = dealt.shape[-1]
    inverse = jnp.zeros((DEVICES,), jnp.int32).at[deal].set(jnp.arange(DEVICES, dtype=jnp.int32))
    blocks = dealt.reshape(DEVICES, TOK_DEV, width)[inverse]
    return blocks.reshape(DEVICES, DEVICES, STRIPE, width).transpose(1, 0, 2, 3).reshape(TOKENS, width)

def block_tables(lengths_row):
    seq_ends = jnp.cumsum(lengths_row).astype(jnp.int32)
    tok_index = jnp.arange(TOK_DEV, dtype=jnp.int32)
    passed = (tok_index[:, None] >= seq_ends[None, :]).astype(jnp.int32)
    segment = lax.optimization_barrier(jnp.sum(passed, axis=1)).astype(jnp.int32)
    seq_start = lax.optimization_barrier(jnp.sum(passed * lengths_row[None, :], axis=1)).astype(jnp.int32)
    return (segment, (tok_index - seq_start).astype(jnp.int32))

def attend(block_parts):
    queries, keys_rot, values_low, segment = block_parts
    factor = HD ** (-0.5)
    scores = low_back(jnp.einsum('thd,shd->hts', queries, keys_rot, precision=lax.Precision.HIGHEST) * factor)
    same_seq = segment[:, None] == segment[None, :]
    scores = jnp.where(same_seq[None], scores, -1e+30)
    row_max = lax.optimization_barrier(jnp.max(scores, axis=-1, keepdims=True))
    weights = jnp.exp(scores - row_max)
    probs = weights / lax.optimization_barrier(jnp.sum(weights, axis=-1, keepdims=True))
    return jnp.einsum('hts,shd->thd', low(probs), values_low, precision=lax.Precision.HIGHEST)

def forward_pass(tokens32, qkv_w, out_w, query_gain, key_gain, attn_gain, ffn_gain, router_w, gate_up_w, down_w, routes, lengths):
    attn_normed = tokens32 * rms_scale(tokens32)
    attn_low = low(attn_normed * attn_gain)
    qkv = low_back(exact_dot(attn_low, qkv_w))
    queries = qkv[:, :D].reshape(TOKENS, H, HD)
    keys_raw = qkv[:, D:2 * D].reshape(TOKENS, H, HD)
    values_low = low(qkv[:, 2 * D:].reshape(TOKENS, H, HD))
    segment, positions = jax.vmap(block_tables)(lengths)
    inverse = jnp.exp(jnp.arange(HD // 2, dtype=jnp.float32) * (-2.0 * math.log(ROPE_BASE) / HD))
    angles = positions.reshape(TOKENS).astype(jnp.float32)[:, None] * inverse[None, :]
    cosine = jnp.cos(angles)[:, None, :]
    sine_part = jnp.sin(angles)[:, None, :]
    queries = low(rotate(queries * rms_scale(queries) * query_gain, cosine, sine_part))
    keys_rot = low(rotate(keys_raw * rms_scale(keys_raw) * key_gain, cosine, sine_part))
    mixed = lax.map(jax.checkpoint(attend), (queries.reshape(DEVICES, TOK_DEV, H, HD), keys_rot.reshape(DEVICES, TOK_DEV, H, HD), values_low.reshape(DEVICES, TOK_DEV, H, HD), segment))
    mixed_low = low(low_back(mixed.reshape(TOKENS, D)))
    residual = tokens32 + low_back(exact_dot(mixed_low, out_w))
    ffn_normed = residual * rms_scale(residual)
    feed_low = low(ffn_normed * ffn_gain)
    logits = exact_dot(feed_low, router_w)
    gates = jax.nn.softmax(jnp.take_along_axis(logits, routes, axis=1), axis=-1)

    def expert_step(moe_total, pieces):
        expert_index, gate_up_one, down_one = pieces
        weight = lax.optimization_barrier(jnp.sum((routes == expert_index).astype(jnp.float32) * gates, axis=1))
        entry_rows = low_back(feed_low)
        gate_up = low_back(exact_dot(entry_rows, gate_up_one))
        inner_low = low(jax.nn.silu(gate_up[:, :FFE]) * gate_up[:, FFE:])
        produced = low(low_back(exact_dot(inner_low, down_one)))
        return (moe_total + weight[:, None] * produced, None)
    moe_sum, _ = lax.scan(jax.checkpoint(expert_step), jnp.zeros((TOKENS, D), jnp.float32), (jnp.arange(EXPERTS, dtype=jnp.int32), gate_up_w, down_w))
    return residual + moe_sum

def reference(tokens, teacher, qkv_weight, out_weight, query_gain, key_gain, attn_gain, ffn_gain, router_weight, gate_up_weight, down_weight, deal, routes, counted, lengths):
    keep_mask = counted.astype(jnp.float32)
    valid_total = jnp.maximum(jnp.sum(keep_mask), 1.0)
    teacher32 = deal_order(teacher.astype(jnp.float32), deal)

    def scaled_loss(tokens32, qkv_w, out_w, q_gain, k_gain, a_gain, f_gain, router_w, gate_up_w, down_w):
        dealt = deal_order(tokens32, deal)
        result = forward_pass(dealt, qkv_w, out_w, q_gain, k_gain, a_gain, f_gain, router_w, gate_up_w, down_w, routes, lengths)
        error_rows = result - teacher32
        squares = jnp.sum(keep_mask[:, None] * error_rows * error_rows)
        return (result, squares * (TOKENS / valid_total))
    params = (tokens.astype(jnp.float32), qkv_weight.astype(jnp.float32), out_weight.astype(jnp.float32), query_gain, key_gain, attn_gain, ffn_gain, router_weight.astype(jnp.float32), gate_up_weight.astype(jnp.float32), down_weight.astype(jnp.float32))
    (result, scaled), pullback = jax.vjp(scaled_loss, *params)
    gradients = pullback((jnp.zeros_like(result), jnp.ones_like(scaled)))
    mean_loss = scaled / (TOKENS * D)
    output = given_order(result, deal).astype(jnp.bfloat16)
    return (output, mean_loss, gradients[0], gradients[1], gradients[2], gradients[3], gradients[4], gradients[5], gradients[6], gradients[7], gradients[8], gradients[9])
```

```python
import math

import jax
import jax.numpy as jnp
from jax import lax
from jax.sharding import PartitionSpec as P

HD = 128
EPS = 1e-06
ROPE_BASE = 50000.0
BOTH = ("dp", "expert")


def rms_scale(values):
    return lax.rsqrt(jnp.mean(values * values, axis=-1, keepdims=True) + EPS)


def rotate(values, cosine, sine_part):
    half = values.shape[-1] // 2
    a, b = values[..., :half], values[..., half:]
    return jnp.concatenate([a * cosine - b * sine_part, b * cosine + a * sine_part], axis=-1)


def norm_back(grad_in, normed, scale_rows):
    return scale_rows * (grad_in - normed * jnp.mean(grad_in * normed, axis=-1, keepdims=True))


def dotf(left, right, dims):
    return lax.dot_general(left, right, (dims, ((), ())), preferred_element_type=jnp.float32)


def swap(pieces, axes):
    return lax.all_to_all(pieces, axes, split_axis=0, concat_axis=0, tiled=True)


def spread(block, axes, count):
    return swap(jnp.broadcast_to(block[None], (count, *block.shape)), axes)


def sum_small(values, devices):
    flat = jnp.concatenate([v.reshape(-1) for v in values])
    size = flat.shape[0]
    chunk = -(-size // (devices * 128)) * 128
    flat = jnp.pad(flat, (0, devices * chunk - size)).reshape(devices, chunk)
    total = jnp.sum(swap(flat, BOTH), axis=0)
    total = spread(total, BOTH, devices).reshape(-1)
    out, at = [], 0
    for v in values:
        out.append(total[at : at + v.size].reshape(v.shape))
        at += v.size
    return out


def on_device(
    tokens,
    teacher,
    qkv_weight,
    out_weight,
    query_gain,
    key_gain,
    attn_gain,
    ffn_gain,
    router_weight,
    gate_up_weight,
    down_weight,
    deal,
    routes,
    counted,
    lengths,
):
    bf16 = jnp.bfloat16
    f32 = jnp.float32
    rows, width = tokens.shape
    slots = routes.shape[1]
    experts = router_weight.shape[1]
    local = gate_up_weight.shape[0]
    hidden = gate_up_weight.shape[2] // 2
    owners = lax.axis_size("expert")
    dps = lax.axis_size("dp")
    devices = dps * owners
    stripe = rows // devices
    my_dp = lax.axis_index("dp")
    my_ex = lax.axis_index("expert")
    part = width // dps
    heads = part // HD
    group = dps * rows
    factor = HD ** (-0.5)

    lanes = 128
    packed = jnp.concatenate(
        [
            routes.reshape(-1),
            counted,
            jnp.pad(lengths[0], (0, lanes - lengths.shape[1])),
        ]
    )
    packed = spread(packed, BOTH, devices)
    packed = packed.reshape(dps, owners, -1)
    total_count = jnp.sum(packed[:, :, rows * slots : rows * slots + rows]).astype(f32)
    valid_total = jnp.maximum(total_count, 1.0)
    group_routes = lax.dynamic_index_in_dim(packed, my_dp, 0, keepdims=False)
    group_routes = group_routes[:, : rows * slots].reshape(owners * rows, slots)
    group_lengths = lax.dynamic_index_in_dim(packed, my_ex, 1, keepdims=False)
    group_lengths = group_lengths[:, rows * slots + rows :][:, : lengths.shape[1]]

    dealt_tokens = swap(tokens.reshape(devices, stripe, width)[deal], BOTH).reshape(rows, width)
    dealt_teacher = swap(teacher.reshape(devices, stripe, width)[deal], BOTH).reshape(rows, width)

    gate_up = []
    for e in range(local):
        gate_up.append(lax.all_gather(gate_up_weight[e], "dp", axis=0, tiled=True))
    down = lax.all_gather(down_weight, "dp", axis=1, tiled=True)
    down = down.reshape(local * hidden, width)

    ends = jnp.cumsum(group_lengths, axis=1)
    index = jnp.arange(rows, dtype=jnp.int32)
    passed = (index[None, :, None] >= ends[:, None, :]).astype(jnp.int32)
    segment = jnp.sum(passed, axis=2)
    start = jnp.sum(passed * group_lengths[:, None, :], axis=2)
    inverse = jnp.exp(
        jnp.arange(HD // 2, dtype=f32) * (-2.0 * math.log(ROPE_BASE) / HD)
    )
    angles = (index[None, :] - start).astype(f32)[:, :, None] * inverse
    cosine = jnp.cos(angles)[:, :, None, :]
    sine_part = jnp.sin(angles)[:, :, None, :]
    same = (segment[:, :, None] == segment[:, None, :])[:, None]

    weight_parts = lax.optimization_barrier(
        jnp.stack(
            [
                jnp.concatenate(
                    [
                        qkv_weight[:, g * width + d * part : g * width + (d + 1) * part]
                        for g in range(3)
                    ],
                    axis=1,
                )
                for d in range(dps)
            ]
        )
    )
    tokens32 = dealt_tokens.astype(f32)
    attn_scale = rms_scale(tokens32)
    attn_normed = tokens32 * attn_scale
    attn_low = (attn_normed * attn_gain).astype(bf16)
    attn_cols = swap(attn_low.reshape(rows, dps, part).transpose(1, 0, 2), "dp")
    attn_cols = attn_cols.reshape(group, part)
    qkv = jnp.einsum("tk,dkc->dtc", attn_cols, weight_parts, preferred_element_type=f32)
    qkv = jnp.sum(swap(qkv.astype(bf16), "dp").astype(f32), axis=0)
    queries, keys, values_low = (
        qkv[:, g * part : (g + 1) * part].reshape(dps, rows, heads, HD) for g in range(3)
    )
    values_low = values_low.astype(bf16)
    query_scale = rms_scale(queries)
    query_normed = queries * query_scale
    query_low = rotate(query_normed * query_gain, cosine, sine_part).astype(bf16)
    key_scale = rms_scale(keys)
    key_normed = keys * key_scale
    key_low = rotate(key_normed * key_gain, cosine, sine_part).astype(bf16)
    scores = (
        jnp.einsum("bthd,bshd->bhts", query_low, key_low, preferred_element_type=f32) * factor
    )
    scores = jnp.where(same, scores, -1e30)
    row_max = jnp.max(scores, axis=-1, keepdims=True)
    weights = jnp.exp(scores - row_max)
    probs = weights / jnp.sum(weights, axis=-1, keepdims=True)
    probs_low = probs.astype(bf16)
    mixed = jnp.einsum("bhts,bshd->bthd", probs_low, values_low, preferred_element_type=f32)
    mixed_low = mixed.reshape(group, part).astype(bf16)
    attn_out = dotf(mixed_low, out_weight, ((1,), (0,)))
    attn_out = swap(attn_out.astype(bf16).reshape(dps, rows, width), "dp")
    residual = tokens32 + jnp.sum(attn_out.astype(f32), axis=0)

    ffn_scale = rms_scale(residual)
    ffn_normed = residual * ffn_scale
    feed_low = (ffn_normed * ffn_gain).astype(bf16)
    feed = lax.all_gather(feed_low, "expert", axis=0, tiled=True)
    logits = dotf(feed, router_weight, ((1,), (0,)))
    table = group_routes[:, :, None] == jnp.arange(experts, dtype=jnp.int32)
    named = jnp.any(table, axis=1)
    masked = jnp.where(named, logits, -jnp.inf)
    gates = jnp.exp(masked - jnp.max(masked, axis=1, keepdims=True))
    gates = gates / jnp.sum(gates, axis=1, keepdims=True)
    own_gates = lax.dynamic_slice_in_dim(gates, my_ex * local, local, axis=1)
    my_gates = lax.dynamic_slice_in_dim(gates, my_ex * rows, rows, axis=0)
    gate_rows, up_rows, inner = [], [], []
    for e in range(local):
        gu = dotf(feed, gate_up[e], ((1,), (0,)))
        g, u = gu[:, :hidden], gu[:, hidden:]
        gate_rows.append(g)
        up_rows.append(u)
        inner.append((jax.nn.silu(g) * u * own_gates[:, e : e + 1]).astype(bf16))
    inner = jnp.concatenate(inner, axis=1)
    moe = dotf(inner, down, ((1,), (0,)))
    moe = lax.psum_scatter(moe.astype(bf16), "expert", scatter_dimension=0, tiled=True)
    result = residual + moe.astype(f32)

    keep = counted.astype(f32)[:, None]
    error_rows = result - dealt_teacher.astype(f32)
    part_square = jnp.sum(keep * error_rows * error_rows)
    grad_result = (2.0 * (rows * devices) / valid_total) * keep * error_rows

    grad_rows = lax.all_gather(grad_result.astype(bf16), "expert", axis=0, tiled=True)
    grad_feed = 0.0
    gate_grads, grad_gate_up_w = [], []
    grad_inner_raw = dotf(grad_rows, down, ((1,), (1,)))
    grad_down_w = dotf(inner, grad_rows, ((0,), (0,)))
    for e in range(local):
        g, u = gate_rows[e], up_rows[e]
        sg = jax.nn.sigmoid(g)
        silu = g * sg
        raw = grad_inner_raw[:, e * hidden : (e + 1) * hidden]
        gate_grads.append(jnp.sum(raw * (silu * u), axis=1))
        grad_inner = raw * own_gates[:, e : e + 1]
        grad_g = grad_inner * u * sg * (1.0 + g * (1.0 - sg))
        grad_u = grad_inner * silu
        grad_gu = jnp.concatenate([grad_g, grad_u], axis=1).astype(bf16)
        grad_gate_up_w.append(dotf(feed, grad_gu, ((0,), (0,))))
        grad_feed = grad_feed + dotf(grad_gu, gate_up[e], ((1,), (1,)))
    grad_feed = lax.psum_scatter(
        grad_feed.astype(bf16), "expert", scatter_dimension=0, tiled=True
    ).astype(f32)
    gate_grad = swap(
        jnp.stack(gate_grads, axis=0).reshape(local, owners, rows).transpose(1, 0, 2), "expert"
    )
    gate_grad = gate_grad.reshape(experts, rows).T
    grad_logits = my_gates * (gate_grad - jnp.sum(my_gates * gate_grad, axis=1, keepdims=True))
    grad_router = lax.dot_general(
        feed_low.astype(f32),
        grad_logits,
        (((0,), (0,)), ((), ())),
        precision=lax.Precision.HIGHEST,
        preferred_element_type=f32,
    )
    grad_feed = grad_feed + lax.dot_general(
        grad_logits,
        router_weight.astype(f32),
        (((1,), (1,)), ((), ())),
        precision=lax.Precision.HIGHEST,
        preferred_element_type=f32,
    )
    grad_ffn_gain = jnp.sum(grad_feed * ffn_normed, axis=0)
    grad_resid = grad_result + norm_back(grad_feed * ffn_gain, ffn_normed, ffn_scale)

    early = sum_small((part_square, grad_ffn_gain, grad_router), devices)
    grad_attn = spread(grad_resid.astype(bf16), "dp", dps).reshape(group, width)
    grad_out_w = dotf(mixed_low, grad_attn, ((0,), (0,)))
    grad_mixed = dotf(grad_attn, out_weight, ((1,), (1,)))
    grad_mixed = grad_mixed.reshape(dps, rows, heads, HD).astype(bf16)
    grad_probs = jnp.einsum("bthd,bshd->bhts", grad_mixed, values_low, preferred_element_type=f32)
    weighted = jnp.sum(probs * grad_probs, axis=-1, keepdims=True)
    grad_scores = (probs * (grad_probs - weighted)).astype(bf16)
    grad_value = jnp.einsum("bhts,bthd->bshd", probs_low, grad_mixed, preferred_element_type=f32)
    grad_query = (
        jnp.einsum("bhts,bshd->bthd", grad_scores, key_low, preferred_element_type=f32) * factor
    )
    grad_key = (
        jnp.einsum("bhts,bthd->bshd", grad_scores, query_low, preferred_element_type=f32) * factor
    )
    grad_qn = rotate(grad_query, cosine, -sine_part)
    grad_query_gain = jnp.sum(grad_qn * query_normed, axis=(0, 1, 2))
    grad_q = norm_back(grad_qn * query_gain, query_normed, query_scale)
    grad_kn = rotate(grad_key, cosine, -sine_part)
    grad_key_gain = jnp.sum(grad_kn * key_normed, axis=(0, 1, 2))
    grad_k = norm_back(grad_kn * key_gain, key_normed, key_scale)
    grad_qkv = jnp.concatenate(
        [
            grad_q.reshape(group, part).astype(bf16),
            grad_k.reshape(group, part).astype(bf16),
            grad_value.reshape(group, part).astype(bf16),
        ],
        axis=1,
    )
    grad_qkv = spread(grad_qkv, "dp", dps)
    grad_qkv_w = [dotf(attn_cols, grad_qkv[d], ((0,), (0,))).astype(bf16) for d in range(dps)]
    grad_qkv_w = jnp.concatenate(
        [grad_qkv_w[d][:, g * part : (g + 1) * part] for g in range(3) for d in range(dps)], axis=1
    )
    grad_normed = jnp.einsum("dtc,dkc->tk", grad_qkv, weight_parts, preferred_element_type=f32)
    grad_normed = swap(grad_normed.astype(bf16).reshape(dps, rows, part), "dp")
    grad_normed = grad_normed.transpose(1, 0, 2).reshape(rows, width).astype(f32)
    grad_attn_gain = jnp.sum(grad_normed * attn_normed, axis=0)
    grad_tokens = grad_resid + norm_back(grad_normed * attn_gain, attn_normed, attn_scale)

    qkv_out = lax.psum_scatter(
        grad_qkv_w, "expert", scatter_dimension=0, tiled=True
    ).astype(f32)
    out_out = lax.psum_scatter(
        grad_out_w.astype(bf16), "expert", scatter_dimension=0, tiled=True
    ).astype(f32)
    gate_up_out = jnp.stack(
        [
            lax.psum_scatter(w.astype(bf16), "dp", scatter_dimension=0, tiled=True).astype(f32)
            for w in grad_gate_up_w
        ]
    )
    down_out = lax.psum_scatter(
        grad_down_w.astype(bf16).reshape(local, hidden, width),
        "dp",
        scatter_dimension=1,
        tiled=True,
    ).astype(f32)
    late = sum_small((grad_query_gain, grad_key_gain, grad_attn_gain), devices)
    mean_loss = early[0] / (valid_total * width)

    inverse_deal = (
        jnp.zeros((devices,), jnp.int32).at[deal].set(jnp.arange(devices, dtype=jnp.int32))
    )
    back_output = swap(result.astype(bf16).reshape(devices, stripe, width), BOTH)
    back_grad = swap(grad_tokens.astype(bf16).reshape(devices, stripe, width), BOTH)
    output = back_output[inverse_deal].reshape(rows, width)
    given_grad = back_grad[inverse_deal].reshape(rows, width).astype(f32)
    return (
        output,
        mean_loss,
        given_grad,
        qkv_out,
        out_out,
        late[0],
        late[1],
        late[2],
        early[1],
        early[2],
        gate_up_out,
        down_out,
    )


def solution(mesh):
    placed = (
        P(BOTH, None),
        P(BOTH, None),
        P("dp", None),
        P("dp", None),
        P(),
        P(),
        P(),
        P(),
        P(),
        P("expert", "dp", None),
        P("expert", "dp", None),
        P(),
        P(BOTH, None),
        P(BOTH),
        P(BOTH, None),
    )
    return jax.shard_map(
        on_device,
        mesh=mesh,
        in_specs=placed,
        out_specs=(
            P(BOTH, None),
            P(),
            P(BOTH, None),
            P(BOTH, None),
            P(BOTH, None),
            P(),
            P(),
            P(),
            P(),
            P(),
            P("expert", "dp", None),
            P("expert", "dp", None),
        ),
        check_vma=False,
    )
```

```python
import functools
import math

import jax
import jax.numpy as jnp
from jax import lax
from jax.experimental import pallas as pl
from jax.experimental.pallas import tpu as pltpu
from jax.sharding import PartitionSpec as P

HD = 128
EPS = 1e-06
ROPE_BASE = 50000.0
BOTH = ("dp", "expert")
LIMIT = 60 * 1024 * 1024


def rms_scale(values):
    return lax.rsqrt(jnp.mean(values * values, axis=-1, keepdims=True) + EPS)


def rotate(values, cosine, sine_part):
    half = values.shape[-1] // 2
    a, b = values[..., :half], values[..., half:]
    return jnp.concatenate([a * cosine - b * sine_part, b * cosine + a * sine_part], axis=-1)


def norm_back(grad_in, normed, scale_rows):
    return scale_rows * (grad_in - normed * jnp.mean(grad_in * normed, axis=-1, keepdims=True))


def dotf(left, right, dims):
    return lax.dot_general(left, right, (dims, ((), ())), preferred_element_type=jnp.float32)


def swap(pieces, axes):
    return lax.all_to_all(pieces, axes, split_axis=0, concat_axis=0, tiled=True)


def spread(block, axes, count):
    return swap(jnp.broadcast_to(block[None], (count, *block.shape)), axes)


def neighbour(index):
    return {"expert": index}


def meet_neighbours(me, count):
    barrier = pltpu.get_barrier_semaphore()

    @pl.when(me > 0)
    def _():
        pl.semaphore_signal(
            barrier, inc=1, device_id=neighbour(me - 1), device_id_type=pl.DeviceIdType.MESH
        )

    @pl.when(me < count - 1)
    def _():
        pl.semaphore_signal(
            barrier, inc=1, device_id=neighbour(me + 1), device_id_type=pl.DeviceIdType.MESH
        )

    ends = ((me == 0) | (me == count - 1)).astype(jnp.int32)
    pl.semaphore_wait(barrier, 2 - ends)


def remote(source, target, send, receive, index):
    return pltpu.make_async_remote_copy(
        src_ref=source,
        dst_ref=target,
        send_sem=send,
        recv_sem=receive,
        device_id=neighbour(index),
        device_id_type=pl.DeviceIdType.MESH,
    )


def gather_kernel(count, block, out, send_right, send_left, receive):
    me = lax.axis_index("expert")
    meet_neighbours(me, count)

    @pl.when(me < count - 1)
    def _():
        remote(block, out.at[me], send_right.at[me], receive.at[me], me + 1).start()

    @pl.when(me > 0)
    def _():
        remote(block, out.at[me], send_left.at[me], receive.at[me], me - 1).start()

    out[me] = block[...]

    def step(s, carry):
        low, high = me - s, me + s

        @pl.when(low >= 0)
        def _():
            remote(out.at[low], out.at[low], send_right.at[low], receive.at[low], me).wait_recv()

            @pl.when(me < count - 1)
            def _():
                remote(
                    out.at[low], out.at[low], send_right.at[low], receive.at[low], me + 1
                ).start()

        @pl.when(high < count)
        def _():
            remote(out.at[high], out.at[high], send_left.at[high], receive.at[high], me).wait_recv()

            @pl.when(me > 0)
            def _():
                remote(
                    out.at[high], out.at[high], send_left.at[high], receive.at[high], me - 1
                ).start()

        return carry

    lax.fori_loop(1, count, step, 0)

    def drain(b, carry):
        @pl.when((b <= me) & (me < count - 1))
        def _():
            remote(block, out.at[b], send_right.at[b], receive.at[b], me + 1).wait_send()

        @pl.when((b >= me) & (me > 0))
        def _():
            remote(block, out.at[b], send_left.at[b], receive.at[b], me - 1).wait_send()

        return carry

    lax.fori_loop(0, count, drain, 0)


def gather_rows(block, number):
    count = lax.axis_size("expert")
    out = pl.pallas_call(
        functools.partial(gather_kernel, count),
        out_shape=jax.ShapeDtypeStruct((count, *block.shape), block.dtype),
        in_specs=[pl.BlockSpec(memory_space=pltpu.VMEM)],
        out_specs=pl.BlockSpec(memory_space=pltpu.VMEM),
        scratch_shapes=[pltpu.SemaphoreType.DMA((count,))] * 3,
        compiler_params=pltpu.CompilerParams(
            collective_id=number, has_side_effects=True, vmem_limit_bytes=LIMIT
        ),
        cost_estimate=pl.CostEstimate(
            flops=0, bytes_accessed=30 * count * block.size, transcendentals=0
        ),
    )(block)
    return out.reshape(count * block.shape[0], *block.shape[1:])


def add_rows(left, right, out):
    rows = out.shape[0]
    step = 16

    def body(r, carry):
        at = pl.ds(pl.multiple_of(r * step, step), step)
        out[at] = (left[at].astype(jnp.float32) + right[at].astype(jnp.float32)).astype(out.dtype)
        return carry

    lax.fori_loop(0, rows // step, body, 0)


def reduce_kernel(
    count, parts, out, right_sums, left_sums, send_right, send_left, receive_right, receive_left
):
    me = lax.axis_index("expert")
    meet_neighbours(me, count)

    def step(t, carry):
        high = count - 1 - (t - me)

        @pl.when((t >= me) & (high > me))
        def _():
            @pl.when(me == 0)
            def _():
                remote(
                    parts.at[high],
                    right_sums.at[high],
                    send_right.at[high],
                    receive_right.at[high],
                    me + 1,
                ).start()

            @pl.when(me > 0)
            def _():
                move = remote(
                    right_sums.at[high],
                    right_sums.at[high],
                    send_right.at[high],
                    receive_right.at[high],
                    me + 1,
                )
                move.wait_recv()
                add_rows(right_sums.at[high], parts.at[high], right_sums.at[high])
                move.start()

        low = t - (count - 1 - me)

        @pl.when((low >= 0) & (low < me))
        def _():
            @pl.when(me == count - 1)
            def _():
                remote(
                    parts.at[low],
                    left_sums.at[low],
                    send_left.at[low],
                    receive_left.at[low],
                    me - 1,
                ).start()

            @pl.when(me < count - 1)
            def _():
                move = remote(
                    left_sums.at[low],
                    left_sums.at[low],
                    send_left.at[low],
                    receive_left.at[low],
                    me - 1,
                )
                move.wait_recv()
                add_rows(left_sums.at[low], parts.at[low], left_sums.at[low])
                move.start()

        return carry

    lax.fori_loop(0, count - 1, step, 0)

    @pl.when(me == 0)
    def _():
        remote(
            left_sums.at[me], left_sums.at[me], send_left.at[me], receive_left.at[me], me
        ).wait_recv()
        add_rows(parts.at[me], left_sums.at[me], out)

    @pl.when(me > 0)
    def _():
        remote(
            right_sums.at[me], right_sums.at[me], send_right.at[me], receive_right.at[me], me
        ).wait_recv()
        add_rows(parts.at[me], right_sums.at[me], out)

        @pl.when(me < count - 1)
        def _():
            remote(
                left_sums.at[me], left_sums.at[me], send_left.at[me], receive_left.at[me], me
            ).wait_recv()
            add_rows(out, left_sums.at[me], out)

    def drain(b, carry):
        @pl.when(b > me)
        def _():
            remote(
                parts.at[b], right_sums.at[b], send_right.at[b], receive_right.at[b], me
            ).wait_send()

        @pl.when(b < me)
        def _():
            remote(
                parts.at[b], left_sums.at[b], send_left.at[b], receive_left.at[b], me
            ).wait_send()

        return carry

    lax.fori_loop(0, count, drain, 0)


def reduce_rows(parts, number):
    count = lax.axis_size("expert")
    parts = parts.reshape(count, -1, parts.shape[-1])
    return pl.pallas_call(
        functools.partial(reduce_kernel, count),
        out_shape=jax.ShapeDtypeStruct(parts.shape[1:], jnp.float32),
        in_specs=[pl.BlockSpec(memory_space=pltpu.VMEM)],
        out_specs=pl.BlockSpec(memory_space=pltpu.VMEM),
        scratch_shapes=[pltpu.VMEM(parts.shape, parts.dtype)] * 2
        + [pltpu.SemaphoreType.DMA((count,))] * 4,
        compiler_params=pltpu.CompilerParams(
            collective_id=number, has_side_effects=True, vmem_limit_bytes=LIMIT
        ),
        cost_estimate=pl.CostEstimate(
            flops=0, bytes_accessed=30 * parts.size, transcendentals=0
        ),
    )(parts)


def sum_small(values, devices):
    flat = jnp.concatenate([v.reshape(-1) for v in values])
    size = flat.shape[0]
    chunk = -(-size // (devices * 128)) * 128
    flat = jnp.pad(flat, (0, devices * chunk - size)).reshape(devices, chunk)
    total = jnp.sum(swap(flat, BOTH), axis=0)
    total = spread(total, BOTH, devices).reshape(-1)
    out, at = [], 0
    for v in values:
        out.append(total[at : at + v.size].reshape(v.shape))
        at += v.size
    return out


def on_device(
    tokens,
    teacher,
    qkv_weight,
    out_weight,
    query_gain,
    key_gain,
    attn_gain,
    ffn_gain,
    router_weight,
    gate_up_weight,
    down_weight,
    deal,
    routes,
    counted,
    lengths,
):
    bf16 = jnp.bfloat16
    f32 = jnp.float32
    rows, width = tokens.shape
    slots = routes.shape[1]
    experts = router_weight.shape[1]
    local = gate_up_weight.shape[0]
    hidden = gate_up_weight.shape[2] // 2
    owners = lax.axis_size("expert")
    dps = lax.axis_size("dp")
    devices = dps * owners
    stripe = rows // devices
    my_dp = lax.axis_index("dp")
    my_ex = lax.axis_index("expert")
    part = width // dps
    piece = part // owners
    heads = part // HD
    group = dps * rows
    factor = HD ** (-0.5)

    lanes = 128
    packed = jnp.concatenate(
        [
            routes.reshape(-1),
            counted,
            jnp.pad(lengths[0], (0, lanes - lengths.shape[1])),
        ]
    )
    packed = spread(packed, BOTH, devices)
    packed = packed.reshape(dps, owners, -1)
    total_count = jnp.sum(packed[:, :, rows * slots : rows * slots + rows]).astype(f32)
    valid_total = jnp.maximum(total_count, 1.0)
    group_routes = lax.dynamic_index_in_dim(packed, my_dp, 0, keepdims=False)
    group_routes = group_routes[:, : rows * slots].reshape(owners * rows, slots)
    group_lengths = lax.dynamic_index_in_dim(packed, my_ex, 1, keepdims=False)
    group_lengths = group_lengths[:, rows * slots + rows :][:, : lengths.shape[1]]

    dealt_tokens = swap(tokens.reshape(devices, stripe, width)[deal], BOTH)
    dealt_tokens = dealt_tokens.reshape(rows, width)
    dealt_teacher = swap(teacher.reshape(devices, stripe, width)[deal], BOTH).reshape(rows, width)

    gate_up = []
    for e in range(local):
        gate_up.append(lax.all_gather(gate_up_weight[e], "dp", axis=0, tiled=True))
    down = lax.all_gather(down_weight, "dp", axis=1, tiled=True)
    down = down.reshape(local * hidden, width)

    ends = jnp.cumsum(group_lengths, axis=1)
    index = jnp.arange(rows, dtype=jnp.int32)
    passed = (index[None, :, None] >= ends[:, None, :]).astype(jnp.int32)
    segment = jnp.sum(passed, axis=2)
    start = jnp.sum(passed * group_lengths[:, None, :], axis=2)
    inverse = jnp.exp(
        jnp.arange(HD // 2, dtype=f32) * (-2.0 * math.log(ROPE_BASE) / HD)
    )
    angles = (index[None, :] - start).astype(f32)[:, :, None] * inverse
    cosine = jnp.cos(angles)[:, :, None, :]
    sine_part = jnp.sin(angles)[:, :, None, :]
    same = (segment[:, :, None] == segment[:, None, :])[:, None]

    mine = lax.dynamic_slice_in_dim(qkv_weight, my_ex * piece, piece, axis=0)
    mine = jnp.stack(
        [
            jnp.concatenate(
                [mine[:, g * width + d * part : g * width + (d + 1) * part] for g in range(3)],
                axis=1,
            )
            for d in range(dps)
        ]
    )
    mine = swap(mine, "dp").reshape(dps * piece, 3 * part)
    weight_cols = gather_rows(mine, 1)
    weight_cols = weight_cols.reshape(owners, dps, piece, 3 * part).transpose(1, 0, 2, 3)
    weight_cols = weight_cols.reshape(width, 3 * part)
    tokens32 = dealt_tokens.astype(f32)
    attn_scale = rms_scale(tokens32)
    attn_normed = tokens32 * attn_scale
    attn_low = (attn_normed * attn_gain).astype(bf16)
    attn_rows = spread(attn_low, "dp", dps).reshape(group, width)
    qkv = dotf(attn_rows, weight_cols, ((1,), (0,)))
    queries, keys, values_low = (
        qkv[:, g * part : (g + 1) * part].reshape(dps, rows, heads, HD) for g in range(3)
    )
    values_low = values_low.astype(bf16)
    query_scale = rms_scale(queries)
    query_normed = queries * query_scale
    query_low = rotate(query_normed * query_gain, cosine, sine_part).astype(bf16)
    key_scale = rms_scale(keys)
    key_normed = keys * key_scale
    key_low = rotate(key_normed * key_gain, cosine, sine_part).astype(bf16)
    scores = (
        jnp.einsum("bthd,bshd->bhts", query_low, key_low, preferred_element_type=f32) * factor
    )
    scores = jnp.where(same, scores, -1e30)
    row_max = jnp.max(scores, axis=-1, keepdims=True)
    weights = jnp.exp(scores - row_max)
    probs = weights / jnp.sum(weights, axis=-1, keepdims=True)
    probs_low = probs.astype(bf16)
    mixed = jnp.einsum("bhts,bshd->bthd", probs_low, values_low, preferred_element_type=f32)
    mixed_low = mixed.reshape(group, part).astype(bf16)
    attn_out = dotf(mixed_low, out_weight, ((1,), (0,)))
    attn_out = swap(attn_out.astype(bf16).reshape(dps, rows, width), "dp")
    residual = tokens32 + jnp.sum(attn_out.astype(f32), axis=0)

    ffn_scale = rms_scale(residual)
    ffn_normed = residual * ffn_scale
    feed_low = (ffn_normed * ffn_gain).astype(bf16)
    feed = gather_rows(feed_low, 2)
    logits = dotf(feed, router_weight, ((1,), (0,)))
    table = group_routes[:, :, None] == jnp.arange(experts, dtype=jnp.int32)
    named = jnp.any(table, axis=1)
    masked = jnp.where(named, logits, -jnp.inf)
    gates = jnp.exp(masked - jnp.max(masked, axis=1, keepdims=True))
    gates = gates / jnp.sum(gates, axis=1, keepdims=True)
    own_gates = lax.dynamic_slice_in_dim(gates, my_ex * local, local, axis=1)
    my_gates = lax.dynamic_slice_in_dim(gates, my_ex * rows, rows, axis=0)
    gate_rows, up_rows, inner = [], [], []
    for e in range(local):
        gu = dotf(feed, gate_up[e], ((1,), (0,)))
        g, u = gu[:, :hidden], gu[:, hidden:]
        gate_rows.append(g)
        up_rows.append(u)
        inner.append((jax.nn.silu(g) * u * own_gates[:, e : e + 1]).astype(bf16))
    inner = jnp.concatenate(inner, axis=1)
    moe = dotf(inner, down, ((1,), (0,)))
    moe = reduce_rows(moe.astype(bf16), 3)
    result = residual + moe

    keep = counted.astype(f32)[:, None]
    error_rows = result - dealt_teacher.astype(f32)
    part_square = jnp.sum(keep * error_rows * error_rows)
    grad_result = (2.0 * (rows * devices) / valid_total) * keep * error_rows

    grad_rows = gather_rows(grad_result.astype(bf16), 4)
    grad_feed = 0.0
    gate_grads, grad_gus = [], []
    grad_inner_raw = dotf(grad_rows, down, ((1,), (1,)))
    for e in range(local):
        g, u = gate_rows[e], up_rows[e]
        sg = jax.nn.sigmoid(g)
        silu = g * sg
        raw = grad_inner_raw[:, e * hidden : (e + 1) * hidden]
        gate_grads.append(jnp.sum(raw * (silu * u), axis=1))
        grad_inner = raw * own_gates[:, e : e + 1]
        grad_g = grad_inner * u * sg * (1.0 + g * (1.0 - sg))
        grad_u = grad_inner * silu
        grad_gu = jnp.concatenate([grad_g, grad_u], axis=1).astype(bf16)
        grad_gus.append(grad_gu)
        grad_feed = grad_feed + dotf(grad_gu, gate_up[e], ((1,), (1,)))
    grad_down_w = dotf(inner, grad_rows, ((0,), (0,))).astype(bf16)
    grad_feed = reduce_rows(grad_feed.astype(bf16), 5)
    grad_gate_up_w = []
    for e in range(local):
        grad_gate_up_w.append(dotf(feed, grad_gus[e], ((0,), (0,))).astype(bf16))
    gate_grad = swap(
        jnp.stack(gate_grads, axis=0).reshape(local, owners, rows).transpose(1, 0, 2), "expert"
    )
    gate_grad = gate_grad.reshape(experts, rows).T
    grad_logits = my_gates * (gate_grad - jnp.sum(my_gates * gate_grad, axis=1, keepdims=True))
    grad_router = lax.dot_general(
        feed_low.astype(f32),
        grad_logits,
        (((0,), (0,)), ((), ())),
        precision=lax.Precision.HIGHEST,
        preferred_element_type=f32,
    )
    grad_feed = grad_feed + lax.dot_general(
        grad_logits,
        router_weight.astype(f32),
        (((1,), (1,)), ((), ())),
        precision=lax.Precision.HIGHEST,
        preferred_element_type=f32,
    )
    grad_ffn_gain = jnp.sum(grad_feed * ffn_normed, axis=0)
    grad_resid = grad_result + norm_back(grad_feed * ffn_gain, ffn_normed, ffn_scale)

    early = sum_small((part_square, grad_ffn_gain, grad_router), devices)
    grad_attn = spread(grad_resid.astype(bf16), "dp", dps)
    grad_attn = grad_attn.reshape(group, width)
    grad_out_w = dotf(mixed_low, grad_attn, ((0,), (0,)))
    grad_mixed = dotf(grad_attn, out_weight, ((1,), (1,)))
    grad_mixed = grad_mixed.reshape(dps, rows, heads, HD).astype(bf16)
    grad_probs = jnp.einsum("bthd,bshd->bhts", grad_mixed, values_low, preferred_element_type=f32)
    weighted = jnp.sum(probs * grad_probs, axis=-1, keepdims=True)
    grad_scores = (probs * (grad_probs - weighted)).astype(bf16)
    grad_value = jnp.einsum("bhts,bthd->bshd", probs_low, grad_mixed, preferred_element_type=f32)
    grad_query = (
        jnp.einsum("bhts,bshd->bthd", grad_scores, key_low, preferred_element_type=f32) * factor
    )
    grad_key = (
        jnp.einsum("bhts,bthd->bshd", grad_scores, query_low, preferred_element_type=f32) * factor
    )
    grad_qn = rotate(grad_query, cosine, -sine_part)
    grad_query_gain = jnp.sum(grad_qn * query_normed, axis=(0, 1, 2))
    grad_q = norm_back(grad_qn * query_gain, query_normed, query_scale)
    grad_kn = rotate(grad_key, cosine, -sine_part)
    grad_key_gain = jnp.sum(grad_kn * key_normed, axis=(0, 1, 2))
    grad_k = norm_back(grad_kn * key_gain, key_normed, key_scale)
    grad_qkv = jnp.concatenate(
        [
            grad_q.reshape(group, part).astype(bf16),
            grad_k.reshape(group, part).astype(bf16),
            grad_value.reshape(group, part).astype(bf16),
        ],
        axis=1,
    )
    grad_normed = dotf(grad_qkv, weight_cols, ((1,), (1,))).astype(bf16)
    grad_normed = swap(grad_normed.reshape(dps, rows, width), "dp")
    grad_normed = jnp.sum(grad_normed.astype(f32), axis=0)
    grad_qkv_w = dotf(attn_rows, grad_qkv, ((0,), (0,))).astype(bf16)
    grad_attn_gain = jnp.sum(grad_normed * attn_normed, axis=0)
    grad_tokens = grad_resid + norm_back(grad_normed * attn_gain, attn_normed, attn_scale)

    grad_qkv_w = grad_qkv_w.reshape(dps, owners, piece, 3 * part).transpose(1, 0, 2, 3)
    grad_qkv_w = reduce_rows(grad_qkv_w.reshape(-1, 3 * part), 6).astype(bf16)
    grad_qkv_w = swap(grad_qkv_w.reshape(dps, piece, 3 * part), "dp")
    qkv_out = jnp.concatenate(
        [grad_qkv_w[d, :, g * part : (g + 1) * part] for g in range(3) for d in range(dps)], axis=1
    ).astype(f32)
    out_out = reduce_rows(grad_out_w.astype(bf16), 7)
    down_out = lax.psum_scatter(
        grad_down_w.reshape(local, hidden, width), "dp", scatter_dimension=1, tiled=True
    )
    down_out = down_out.astype(f32)
    gate_up_out = []
    for e in range(local):
        gate_up_out.append(
            lax.psum_scatter(grad_gate_up_w[e], "dp", scatter_dimension=0, tiled=True)
        )
    gate_up_out = jnp.stack([w.astype(f32) for w in gate_up_out])
    late = sum_small((grad_query_gain, grad_key_gain, grad_attn_gain), devices)
    mean_loss = early[0] / (valid_total * width)

    inverse_deal = (
        jnp.zeros((devices,), jnp.int32).at[deal].set(jnp.arange(devices, dtype=jnp.int32))
    )
    back_output = swap(result.astype(bf16).reshape(devices, stripe, width), BOTH)
    back_grad = swap(grad_tokens.astype(bf16).reshape(devices, stripe, width), BOTH)
    output = back_output[inverse_deal].reshape(rows, width)
    given_grad = back_grad[inverse_deal].reshape(rows, width).astype(f32)
    return (
        output,
        mean_loss,
        given_grad,
        qkv_out,
        out_out,
        late[0],
        late[1],
        late[2],
        early[1],
        early[2],
        gate_up_out,
        down_out,
    )


def solution(mesh):
    placed = (
        P(BOTH, None),
        P(BOTH, None),
        P("dp", None),
        P("dp", None),
        P(),
        P(),
        P(),
        P(),
        P(),
        P("expert", "dp", None),
        P("expert", "dp", None),
        P(),
        P(BOTH, None),
        P(BOTH),
        P(BOTH, None),
    )
    return jax.shard_map(
        on_device,
        mesh=mesh,
        in_specs=placed,
        out_specs=(
            P(BOTH, None),
            P(),
            P(BOTH, None),
            P(BOTH, None),
            P(BOTH, None),
            P(),
            P(),
            P(),
            P(),
            P(),
            P("expert", "dp", None),
            P("expert", "dp", None),
        ),
        check_vma=False,
    )
```

```python
import functools
import math

import jax
import jax.numpy as jnp
from jax import lax
from jax.experimental import pallas as pl
from jax.experimental.pallas import tpu as pltpu
from jax.sharding import PartitionSpec as P

HD = 128
EPS = 1e-06
ROPE_BASE = 50000.0
BOTH = ("dp", "expert")
LIMIT = 60 * 1024 * 1024


def rms_scale(values):
    return lax.rsqrt(jnp.mean(values * values, axis=-1, keepdims=True) + EPS)


def rotate(values, cosine, sine_part):
    half = values.shape[-1] // 2
    a, b = values[..., :half], values[..., half:]
    return jnp.concatenate([a * cosine - b * sine_part, b * cosine + a * sine_part], axis=-1)


def norm_back(grad_in, normed, scale_rows):
    return scale_rows * (grad_in - normed * jnp.mean(grad_in * normed, axis=-1, keepdims=True))


def dotf(left, right, dims):
    return lax.dot_general(left, right, (dims, ((), ())), preferred_element_type=jnp.float32)


def swap(pieces, axes):
    return lax.all_to_all(pieces, axes, split_axis=0, concat_axis=0, tiled=True)


def spread(block, axes, count):
    return swap(jnp.broadcast_to(block[None], (count, *block.shape)), axes)


def neighbour(index):
    return {"expert": index}


def meet_neighbours(me, count):
    barrier = pltpu.get_barrier_semaphore()

    @pl.when(me > 0)
    def _():
        pl.semaphore_signal(
            barrier, inc=1, device_id=neighbour(me - 1), device_id_type=pl.DeviceIdType.MESH
        )

    @pl.when(me < count - 1)
    def _():
        pl.semaphore_signal(
            barrier, inc=1, device_id=neighbour(me + 1), device_id_type=pl.DeviceIdType.MESH
        )

    ends = ((me == 0) | (me == count - 1)).astype(jnp.int32)
    pl.semaphore_wait(barrier, 2 - ends)


def remote(source, target, send, receive, index):
    return pltpu.make_async_remote_copy(
        src_ref=source,
        dst_ref=target,
        send_sem=send,
        recv_sem=receive,
        device_id=neighbour(index),
        device_id_type=pl.DeviceIdType.MESH,
    )


def gather_kernel(count, block, out, send_right, send_left, receive):
    me = lax.axis_index("expert")
    meet_neighbours(me, count)

    @pl.when(me < count - 1)
    def _():
        remote(block, out.at[me], send_right.at[me], receive.at[me], me + 1).start()

    @pl.when(me > 0)
    def _():
        remote(block, out.at[me], send_left.at[me], receive.at[me], me - 1).start()

    out[me] = block[...]

    def step(s, carry):
        low, high = me - s, me + s

        @pl.when(low >= 0)
        def _():
            remote(out.at[low], out.at[low], send_right.at[low], receive.at[low], me).wait_recv()

            @pl.when(me < count - 1)
            def _():
                remote(
                    out.at[low], out.at[low], send_right.at[low], receive.at[low], me + 1
                ).start()

        @pl.when(high < count)
        def _():
            remote(out.at[high], out.at[high], send_left.at[high], receive.at[high], me).wait_recv()

            @pl.when(me > 0)
            def _():
                remote(
                    out.at[high], out.at[high], send_left.at[high], receive.at[high], me - 1
                ).start()

        return carry

    lax.fori_loop(1, count, step, 0)

    def drain(b, carry):
        @pl.when((b <= me) & (me < count - 1))
        def _():
            remote(block, out.at[b], send_right.at[b], receive.at[b], me + 1).wait_send()

        @pl.when((b >= me) & (me > 0))
        def _():
            remote(block, out.at[b], send_left.at[b], receive.at[b], me - 1).wait_send()

        return carry

    lax.fori_loop(0, count, drain, 0)


def gather_rows(block, number):
    count = lax.axis_size("expert")
    out = pl.pallas_call(
        functools.partial(gather_kernel, count),
        out_shape=jax.ShapeDtypeStruct((count, *block.shape), block.dtype),
        in_specs=[pl.BlockSpec(memory_space=pltpu.VMEM)],
        out_specs=pl.BlockSpec(memory_space=pltpu.VMEM),
        scratch_shapes=[pltpu.SemaphoreType.DMA((count,))] * 3,
        compiler_params=pltpu.CompilerParams(
            collective_id=number, has_side_effects=True, vmem_limit_bytes=LIMIT
        ),
        cost_estimate=pl.CostEstimate(
            flops=0, bytes_accessed=30 * count * block.size, transcendentals=0
        ),
    )(block)
    return out.reshape(count * block.shape[0], *block.shape[1:])


def add_rows(left, right, out):
    rows = out.shape[0]
    step = 16

    def body(r, carry):
        at = pl.ds(pl.multiple_of(r * step, step), step)
        out[at] = (left[at].astype(jnp.float32) + right[at].astype(jnp.float32)).astype(out.dtype)
        return carry

    lax.fori_loop(0, rows // step, body, 0)


def reduce_kernel(
    count, parts, out, right_sums, left_sums, send_right, send_left, receive_right, receive_left
):
    me = lax.axis_index("expert")
    meet_neighbours(me, count)

    def step(t, carry):
        high = count - 1 - (t - me)

        @pl.when((t >= me) & (high > me))
        def _():
            @pl.when(me == 0)
            def _():
                remote(
                    parts.at[high],
                    right_sums.at[high],
                    send_right.at[high],
                    receive_right.at[high],
                    me + 1,
                ).start()

            @pl.when(me > 0)
            def _():
                move = remote(
                    right_sums.at[high],
                    right_sums.at[high],
                    send_right.at[high],
                    receive_right.at[high],
                    me + 1,
                )
                move.wait_recv()
                add_rows(right_sums.at[high], parts.at[high], right_sums.at[high])
                move.start()

        low = t - (count - 1 - me)

        @pl.when((low >= 0) & (low < me))
        def _():
            @pl.when(me == count - 1)
            def _():
                remote(
                    parts.at[low],
                    left_sums.at[low],
                    send_left.at[low],
                    receive_left.at[low],
                    me - 1,
                ).start()

            @pl.when(me < count - 1)
            def _():
                move = remote(
                    left_sums.at[low],
                    left_sums.at[low],
                    send_left.at[low],
                    receive_left.at[low],
                    me - 1,
                )
                move.wait_recv()
                add_rows(left_sums.at[low], parts.at[low], left_sums.at[low])
                move.start()

        return carry

    lax.fori_loop(0, count - 1, step, 0)

    @pl.when(me == 0)
    def _():
        remote(
            left_sums.at[me], left_sums.at[me], send_left.at[me], receive_left.at[me], me
        ).wait_recv()
        add_rows(parts.at[me], left_sums.at[me], out)

    @pl.when(me > 0)
    def _():
        remote(
            right_sums.at[me], right_sums.at[me], send_right.at[me], receive_right.at[me], me
        ).wait_recv()
        add_rows(parts.at[me], right_sums.at[me], out)

        @pl.when(me < count - 1)
        def _():
            remote(
                left_sums.at[me], left_sums.at[me], send_left.at[me], receive_left.at[me], me
            ).wait_recv()
            add_rows(out, left_sums.at[me], out)

    def drain(b, carry):
        @pl.when(b > me)
        def _():
            remote(
                parts.at[b], right_sums.at[b], send_right.at[b], receive_right.at[b], me
            ).wait_send()

        @pl.when(b < me)
        def _():
            remote(
                parts.at[b], left_sums.at[b], send_left.at[b], receive_left.at[b], me
            ).wait_send()

        return carry

    lax.fori_loop(0, count, drain, 0)


def reduce_rows(parts, number):
    count = lax.axis_size("expert")
    parts = parts.reshape(count, -1, parts.shape[-1])
    return pl.pallas_call(
        functools.partial(reduce_kernel, count),
        out_shape=jax.ShapeDtypeStruct(parts.shape[1:], jnp.float32),
        in_specs=[pl.BlockSpec(memory_space=pltpu.VMEM)],
        out_specs=pl.BlockSpec(memory_space=pltpu.VMEM),
        scratch_shapes=[pltpu.VMEM(parts.shape, parts.dtype)] * 2
        + [pltpu.SemaphoreType.DMA((count,))] * 4,
        compiler_params=pltpu.CompilerParams(
            collective_id=number, has_side_effects=True, vmem_limit_bytes=LIMIT
        ),
        cost_estimate=pl.CostEstimate(
            flops=0, bytes_accessed=30 * parts.size, transcendentals=0
        ),
    )(parts)


def sum_small(values, devices):
    flat = jnp.concatenate([v.reshape(-1) for v in values])
    size = flat.shape[0]
    chunk = -(-size // (devices * 128)) * 128
    flat = jnp.pad(flat, (0, devices * chunk - size)).reshape(devices, chunk)
    total = jnp.sum(swap(flat, BOTH), axis=0)
    total = spread(total, BOTH, devices).reshape(-1)
    out, at = [], 0
    for v in values:
        out.append(total[at : at + v.size].reshape(v.shape))
        at += v.size
    return out


def on_device(
    tokens,
    teacher,
    qkv_weight,
    out_weight,
    query_gain,
    key_gain,
    attn_gain,
    ffn_gain,
    router_weight,
    gate_up_weight,
    down_weight,
    deal,
    routes,
    counted,
    lengths,
):
    bf16 = jnp.bfloat16
    f32 = jnp.float32
    rows, width = tokens.shape
    slots = routes.shape[1]
    experts = router_weight.shape[1]
    local = gate_up_weight.shape[0]
    hidden = gate_up_weight.shape[2] // 2
    owners = lax.axis_size("expert")
    dps = lax.axis_size("dp")
    devices = dps * owners
    stripe = rows // devices
    my_dp = lax.axis_index("dp")
    my_ex = lax.axis_index("expert")
    part = width // dps
    piece = part // owners
    heads = part // HD
    group = dps * rows
    factor = HD ** (-0.5)

    lanes = 128
    packed = jnp.concatenate(
        [
            routes.reshape(-1),
            counted,
            jnp.pad(lengths[0], (0, lanes - lengths.shape[1])),
        ]
    )
    packed = spread(packed, BOTH, devices)
    packed = packed.reshape(dps, owners, -1)
    total_count = jnp.sum(packed[:, :, rows * slots : rows * slots + rows]).astype(f32)
    valid_total = jnp.maximum(total_count, 1.0)
    group_routes = lax.dynamic_index_in_dim(packed, my_dp, 0, keepdims=False)
    group_routes = group_routes[:, : rows * slots].reshape(owners * rows, slots)
    group_lengths = lax.dynamic_index_in_dim(packed, my_ex, 1, keepdims=False)
    group_lengths = group_lengths[:, rows * slots + rows :][:, : lengths.shape[1]]

    dealt_tokens = swap(tokens.reshape(devices, stripe, width)[deal], BOTH)
    dealt_tokens = dealt_tokens.reshape(rows, width)
    dealt_teacher = swap(teacher.reshape(devices, stripe, width)[deal], BOTH).reshape(rows, width)

    gate_up = []
    for e in range(local):
        gate_up.append(lax.all_gather(gate_up_weight[e], "dp", axis=0, tiled=True))
    down = lax.all_gather(down_weight, "dp", axis=1, tiled=True)
    down = down.reshape(local * hidden, width)

    ends = jnp.cumsum(group_lengths, axis=1)
    index = jnp.arange(rows, dtype=jnp.int32)
    passed = (index[None, :, None] >= ends[:, None, :]).astype(jnp.int32)
    segment = jnp.sum(passed, axis=2)
    start = jnp.sum(passed * group_lengths[:, None, :], axis=2)
    inverse = jnp.exp(
        jnp.arange(HD // 2, dtype=f32) * (-2.0 * math.log(ROPE_BASE) / HD)
    )
    angles = (index[None, :] - start).astype(f32)[:, :, None] * inverse
    cosine = jnp.cos(angles)[:, :, None, :]
    sine_part = jnp.sin(angles)[:, :, None, :]
    same = (segment[:, :, None] == segment[:, None, :])[:, None]

    mine = lax.dynamic_slice_in_dim(qkv_weight, my_ex * piece, piece, axis=0)
    mine = jnp.stack(
        [
            jnp.concatenate(
                [mine[:, g * width + d * part : g * width + (d + 1) * part] for g in range(3)],
                axis=1,
            )
            for d in range(dps)
        ]
    )
    mine = swap(mine, "dp").reshape(dps * piece, 3 * part)
    weight_cols = gather_rows(mine, 1)
    weight_cols = weight_cols.reshape(owners, dps, piece, 3 * part).transpose(1, 0, 2, 3)
    weight_cols = weight_cols.reshape(width, 3 * part)
    tokens32 = dealt_tokens.astype(f32)
    attn_scale = rms_scale(tokens32)
    attn_normed = tokens32 * attn_scale
    attn_low = (attn_normed * attn_gain).astype(bf16)
    attn_rows = spread(attn_low, "dp", dps).reshape(group, width)
    qkv = dotf(attn_rows, weight_cols, ((1,), (0,)))
    queries, keys, values_low = (
        qkv[:, g * part : (g + 1) * part].reshape(dps, rows, heads, HD) for g in range(3)
    )
    values_low = values_low.astype(bf16)
    query_scale = rms_scale(queries)
    query_normed = queries * query_scale
    query_low = rotate(query_normed * query_gain, cosine, sine_part).astype(bf16)
    key_scale = rms_scale(keys)
    key_normed = keys * key_scale
    key_low = rotate(key_normed * key_gain, cosine, sine_part).astype(bf16)
    scores = (
        jnp.einsum("bthd,bshd->bhts", query_low, key_low, preferred_element_type=f32) * factor
    )
    scores = jnp.where(same, scores, -1e30)
    row_max = jnp.max(scores, axis=-1, keepdims=True)
    weights = jnp.exp(scores - row_max)
    probs = weights / jnp.sum(weights, axis=-1, keepdims=True)
    probs_low = probs.astype(bf16)
    mixed = jnp.einsum("bhts,bshd->bthd", probs_low, values_low, preferred_element_type=f32)
    mixed_low = mixed.reshape(group, part).astype(bf16)
    attn_out = dotf(mixed_low, out_weight, ((1,), (0,)))
    attn_out = swap(attn_out.astype(bf16).reshape(dps, rows, width), "dp")
    residual = tokens32 + jnp.sum(attn_out.astype(f32), axis=0)

    ffn_scale = rms_scale(residual)
    ffn_normed = residual * ffn_scale
    feed_low = (ffn_normed * ffn_gain).astype(bf16)
    feed = gather_rows(feed_low, 2)
    logits = dotf(feed, router_weight, ((1,), (0,)))
    table = group_routes[:, :, None] == jnp.arange(experts, dtype=jnp.int32)
    named = jnp.any(table, axis=1)
    masked = jnp.where(named, logits, -jnp.inf)
    gates = jnp.exp(masked - jnp.max(masked, axis=1, keepdims=True))
    gates = gates / jnp.sum(gates, axis=1, keepdims=True)
    own_gates = lax.dynamic_slice_in_dim(gates, my_ex * local, local, axis=1)
    my_gates = lax.dynamic_slice_in_dim(gates, my_ex * rows, rows, axis=0)
    gate_rows, up_rows, inner = [], [], []
    for e in range(local):
        gu = dotf(feed, gate_up[e], ((1,), (0,)))
        g, u = gu[:, :hidden], gu[:, hidden:]
        gate_rows.append(g)
        up_rows.append(u)
        inner.append((jax.nn.silu(g) * u * own_gates[:, e : e + 1]).astype(bf16))
    inner = jnp.concatenate(inner, axis=1)
    moe = dotf(inner, down, ((1,), (0,)))
    moe = reduce_rows(moe.astype(bf16), 3)
    result = residual + moe

    keep = counted.astype(f32)[:, None]
    error_rows = result - dealt_teacher.astype(f32)
    part_square = jnp.sum(keep * error_rows * error_rows)
    grad_result = (2.0 * (rows * devices) / valid_total) * keep * error_rows

    grad_rows = gather_rows(grad_result.astype(bf16), 4)
    output_rows, grad_rows = lax.optimization_barrier((result.astype(bf16), grad_rows))
    back_output = swap(output_rows.reshape(devices, stripe, width), BOTH)
    grad_feed = 0.0
    gate_grads, grad_gus = [], []
    grad_inner_raw = dotf(grad_rows, down, ((1,), (1,)))
    for e in range(local):
        g, u = gate_rows[e], up_rows[e]
        sg = jax.nn.sigmoid(g)
        silu = g * sg
        raw = grad_inner_raw[:, e * hidden : (e + 1) * hidden]
        gate_grads.append(jnp.sum(raw * (silu * u), axis=1))
        grad_inner = raw * own_gates[:, e : e + 1]
        grad_g = grad_inner * u * sg * (1.0 + g * (1.0 - sg))
        grad_u = grad_inner * silu
        grad_gu = jnp.concatenate([grad_g, grad_u], axis=1).astype(bf16)
        grad_gus.append(grad_gu)
        grad_feed = grad_feed + dotf(grad_gu, gate_up[e], ((1,), (1,)))
    grad_down_w = dotf(inner, grad_rows, ((0,), (0,))).astype(bf16)
    grad_feed = reduce_rows(grad_feed.astype(bf16), 5)
    grad_gate_up_w = []
    for e in range(local):
        grad_gate_up_w.append(dotf(feed, grad_gus[e], ((0,), (0,))).astype(bf16))
    gate_grad = swap(
        jnp.stack(gate_grads, axis=0).reshape(local, owners, rows).transpose(1, 0, 2), "expert"
    )
    gate_grad = gate_grad.reshape(experts, rows).T
    grad_logits = my_gates * (gate_grad - jnp.sum(my_gates * gate_grad, axis=1, keepdims=True))
    grad_router = lax.dot_general(
        feed_low.astype(f32),
        grad_logits,
        (((0,), (0,)), ((), ())),
        precision=lax.Precision.HIGHEST,
        preferred_element_type=f32,
    )
    grad_feed = grad_feed + lax.dot_general(
        grad_logits,
        router_weight.astype(f32),
        (((1,), (1,)), ((), ())),
        precision=lax.Precision.HIGHEST,
        preferred_element_type=f32,
    )
    grad_ffn_gain = jnp.sum(grad_feed * ffn_normed, axis=0)
    grad_resid = grad_result + norm_back(grad_feed * ffn_gain, ffn_normed, ffn_scale)

    grad_attn = spread(grad_resid.astype(bf16), "dp", dps)
    grad_attn = grad_attn.reshape(group, width)
    grad_out_w = dotf(mixed_low, grad_attn, ((0,), (0,))).astype(bf16)
    grad_mixed = dotf(grad_attn, out_weight, ((1,), (1,)))
    grad_mixed = grad_mixed.reshape(dps, rows, heads, HD).astype(bf16)
    grad_probs = jnp.einsum("bthd,bshd->bhts", grad_mixed, values_low, preferred_element_type=f32)
    weighted = jnp.sum(probs * grad_probs, axis=-1, keepdims=True)
    grad_scores = (probs * (grad_probs - weighted)).astype(bf16)
    grad_value = jnp.einsum("bhts,bthd->bshd", probs_low, grad_mixed, preferred_element_type=f32)
    grad_query = (
        jnp.einsum("bhts,bshd->bthd", grad_scores, key_low, preferred_element_type=f32) * factor
    )
    grad_key = (
        jnp.einsum("bhts,bthd->bshd", grad_scores, query_low, preferred_element_type=f32) * factor
    )
    grad_qn = rotate(grad_query, cosine, -sine_part)
    grad_query_gain = jnp.sum(grad_qn * query_normed, axis=(0, 1, 2))
    grad_q = norm_back(grad_qn * query_gain, query_normed, query_scale)
    grad_kn = rotate(grad_key, cosine, -sine_part)
    grad_key_gain = jnp.sum(grad_kn * key_normed, axis=(0, 1, 2))
    grad_k = norm_back(grad_kn * key_gain, key_normed, key_scale)
    grad_qkv = jnp.concatenate(
        [
            grad_q.reshape(group, part).astype(bf16),
            grad_k.reshape(group, part).astype(bf16),
            grad_value.reshape(group, part).astype(bf16),
        ],
        axis=1,
    )
    grad_normed = dotf(grad_qkv, weight_cols, ((1,), (1,))).astype(bf16)
    grad_normed = swap(grad_normed.reshape(dps, rows, width), "dp")
    grad_normed = jnp.sum(grad_normed.astype(f32), axis=0)
    grad_qkv_w = dotf(attn_rows, grad_qkv, ((0,), (0,))).astype(bf16)
    grad_attn_gain = jnp.sum(grad_normed * attn_normed, axis=0)
    grad_tokens = grad_resid + norm_back(grad_normed * attn_gain, attn_normed, attn_scale)

    grad_qkv_w = grad_qkv_w.reshape(dps, owners, piece, 3, part).transpose(1, 3, 2, 0, 4)
    attn_grads = jnp.concatenate(
        [
            grad_qkv_w.reshape(owners, 3 * piece, width),
            grad_out_w.reshape(owners, piece, width),
        ],
        axis=1,
    )
    attn_grads = reduce_rows(attn_grads.reshape(-1, width), 6)
    out_out = attn_grads[3 * piece :]
    grad_qkv_w = attn_grads[: 3 * piece].astype(bf16).reshape(3 * piece, dps, part)
    grad_qkv_w = swap(grad_qkv_w.transpose(1, 0, 2), "dp")
    qkv_out = jnp.concatenate(
        [grad_qkv_w[d, g * piece : (g + 1) * piece] for g in range(3) for d in range(dps)], axis=1
    ).astype(f32)
    down_out = lax.psum_scatter(
        grad_down_w.reshape(local, hidden, width), "dp", scatter_dimension=1, tiled=True
    )
    down_out = down_out.astype(f32)
    gate_up_out = []
    for e in range(local):
        gate_up_out.append(
            lax.psum_scatter(grad_gate_up_w[e], "dp", scatter_dimension=0, tiled=True)
        )
    gate_up_out = jnp.stack([w.astype(f32) for w in gate_up_out])
    sums = sum_small(
        (part_square, grad_query_gain, grad_key_gain, grad_attn_gain, grad_ffn_gain, grad_router),
        devices,
    )
    mean_loss = sums[0] / (valid_total * width)

    inverse_deal = (
        jnp.zeros((devices,), jnp.int32).at[deal].set(jnp.arange(devices, dtype=jnp.int32))
    )
    back_grad = swap(grad_tokens.astype(bf16).reshape(devices, stripe, width), BOTH)
    output = back_output[inverse_deal].reshape(rows, width)
    given_grad = back_grad[inverse_deal].reshape(rows, width).astype(f32)
    return (
        output,
        mean_loss,
        given_grad,
        qkv_out,
        out_out,
        sums[1],
        sums[2],
        sums[3],
        sums[4],
        sums[5],
        gate_up_out,
        down_out,
    )


def solution(mesh):
    placed = (
        P(BOTH, None),
        P(BOTH, None),
        P("dp", None),
        P("dp", None),
        P(),
        P(),
        P(),
        P(),
        P(),
        P("expert", "dp", None),
        P("expert", "dp", None),
        P(),
        P(BOTH, None),
        P(BOTH),
        P(BOTH, None),
    )
    return jax.shard_map(
        on_device,
        mesh=mesh,
        in_specs=placed,
        out_specs=(
            P(BOTH, None),
            P(),
            P(BOTH, None),
            P(BOTH, None),
            P(BOTH, None),
            P(),
            P(),
            P(),
            P(),
            P(),
            P("expert", "dp", None),
            P("expert", "dp", None),
        ),
        check_vma=False,
    )
```

```python
import functools
import math

import jax
import jax.numpy as jnp
from jax import lax
from jax.experimental import pallas as pl
from jax.experimental.pallas import tpu as pltpu
from jax.sharding import PartitionSpec as P

HD = 128
EPS = 1e-06
ROPE_BASE = 50000.0
BOTH = ("dp", "expert")
LIMIT = 60 * 1024 * 1024


def rms_scale(values):
    return lax.rsqrt(jnp.mean(values * values, axis=-1, keepdims=True) + EPS)


def rotate(values, cosine, sine_part):
    half = values.shape[-1] // 2
    a, b = values[..., :half], values[..., half:]
    return jnp.concatenate([a * cosine - b * sine_part, b * cosine + a * sine_part], axis=-1)


def norm_back(grad_in, normed, scale_rows):
    return scale_rows * (grad_in - normed * jnp.mean(grad_in * normed, axis=-1, keepdims=True))


def dotf(left, right, dims):
    return lax.dot_general(left, right, (dims, ((), ())), preferred_element_type=jnp.float32)


def swap(pieces, axes):
    return lax.all_to_all(pieces, axes, split_axis=0, concat_axis=0, tiled=True)


def spread(block, axes, count):
    return swap(jnp.broadcast_to(block[None], (count, *block.shape)), axes)


def neighbour(index):
    return {"expert": index}


def meet_neighbours(me, count):
    barrier = pltpu.get_barrier_semaphore()

    @pl.when(me > 0)
    def _():
        pl.semaphore_signal(
            barrier, inc=1, device_id=neighbour(me - 1), device_id_type=pl.DeviceIdType.MESH
        )

    @pl.when(me < count - 1)
    def _():
        pl.semaphore_signal(
            barrier, inc=1, device_id=neighbour(me + 1), device_id_type=pl.DeviceIdType.MESH
        )

    ends = ((me == 0) | (me == count - 1)).astype(jnp.int32)
    pl.semaphore_wait(barrier, 2 - ends)


def remote(source, target, send, receive, index):
    return pltpu.make_async_remote_copy(
        src_ref=source,
        dst_ref=target,
        send_sem=send,
        recv_sem=receive,
        device_id=neighbour(index),
        device_id_type=pl.DeviceIdType.MESH,
    )


def gather_kernel(count, block, out, send_right, send_left, receive):
    me = lax.axis_index("expert")
    meet_neighbours(me, count)

    @pl.when(me < count - 1)
    def _():
        remote(block, out.at[me], send_right.at[me], receive.at[me], me + 1).start()

    @pl.when(me > 0)
    def _():
        remote(block, out.at[me], send_left.at[me], receive.at[me], me - 1).start()

    out[me] = block[...]

    def step(s, carry):
        low, high = me - s, me + s

        @pl.when(low >= 0)
        def _():
            remote(out.at[low], out.at[low], send_right.at[low], receive.at[low], me).wait_recv()

            @pl.when(me < count - 1)
            def _():
                remote(
                    out.at[low], out.at[low], send_right.at[low], receive.at[low], me + 1
                ).start()

        @pl.when(high < count)
        def _():
            remote(out.at[high], out.at[high], send_left.at[high], receive.at[high], me).wait_recv()

            @pl.when(me > 0)
            def _():
                remote(
                    out.at[high], out.at[high], send_left.at[high], receive.at[high], me - 1
                ).start()

        return carry

    lax.fori_loop(1, count, step, 0)

    def drain(b, carry):
        @pl.when((b <= me) & (me < count - 1))
        def _():
            remote(block, out.at[b], send_right.at[b], receive.at[b], me + 1).wait_send()

        @pl.when((b >= me) & (me > 0))
        def _():
            remote(block, out.at[b], send_left.at[b], receive.at[b], me - 1).wait_send()

        return carry

    lax.fori_loop(0, count, drain, 0)


def gather_rows(block, number):
    count = lax.axis_size("expert")
    out = pl.pallas_call(
        functools.partial(gather_kernel, count),
        out_shape=jax.ShapeDtypeStruct((count, *block.shape), block.dtype),
        in_specs=[pl.BlockSpec(memory_space=pltpu.VMEM)],
        out_specs=pl.BlockSpec(memory_space=pltpu.VMEM),
        scratch_shapes=[pltpu.SemaphoreType.DMA((count,))] * 3,
        compiler_params=pltpu.CompilerParams(
            collective_id=number, has_side_effects=True, vmem_limit_bytes=LIMIT
        ),
        cost_estimate=pl.CostEstimate(
            flops=0, bytes_accessed=30 * count * block.size, transcendentals=0
        ),
    )(block)
    return out.reshape(count * block.shape[0], *block.shape[1:])


def add_rows(left, right, out):
    rows = out.shape[0]
    step = 16

    def body(r, carry):
        at = pl.ds(pl.multiple_of(r * step, step), step)
        out[at] = (left[at].astype(jnp.float32) + right[at].astype(jnp.float32)).astype(out.dtype)
        return carry

    lax.fori_loop(0, rows // step, body, 0)


def reduce_kernel(
    count, parts, out, right_sums, left_sums, send_right, send_left, receive_right, receive_left
):
    me = lax.axis_index("expert")
    meet_neighbours(me, count)

    def step(t, carry):
        high = count - 1 - (t - me)

        @pl.when((t >= me) & (high > me))
        def _():
            @pl.when(me == 0)
            def _():
                remote(
                    parts.at[high],
                    right_sums.at[high],
                    send_right.at[high],
                    receive_right.at[high],
                    me + 1,
                ).start()

            @pl.when(me > 0)
            def _():
                move = remote(
                    right_sums.at[high],
                    right_sums.at[high],
                    send_right.at[high],
                    receive_right.at[high],
                    me + 1,
                )
                move.wait_recv()
                add_rows(right_sums.at[high], parts.at[high], right_sums.at[high])
                move.start()

        low = t - (count - 1 - me)

        @pl.when((low >= 0) & (low < me))
        def _():
            @pl.when(me == count - 1)
            def _():
                remote(
                    parts.at[low],
                    left_sums.at[low],
                    send_left.at[low],
                    receive_left.at[low],
                    me - 1,
                ).start()

            @pl.when(me < count - 1)
            def _():
                move = remote(
                    left_sums.at[low],
                    left_sums.at[low],
                    send_left.at[low],
                    receive_left.at[low],
                    me - 1,
                )
                move.wait_recv()
                add_rows(left_sums.at[low], parts.at[low], left_sums.at[low])
                move.start()

        return carry

    lax.fori_loop(0, count - 1, step, 0)

    @pl.when(me == 0)
    def _():
        remote(
            left_sums.at[me], left_sums.at[me], send_left.at[me], receive_left.at[me], me
        ).wait_recv()
        add_rows(parts.at[me], left_sums.at[me], out)

    @pl.when(me > 0)
    def _():
        remote(
            right_sums.at[me], right_sums.at[me], send_right.at[me], receive_right.at[me], me
        ).wait_recv()
        add_rows(parts.at[me], right_sums.at[me], out)

        @pl.when(me < count - 1)
        def _():
            remote(
                left_sums.at[me], left_sums.at[me], send_left.at[me], receive_left.at[me], me
            ).wait_recv()
            add_rows(out, left_sums.at[me], out)

    def drain(b, carry):
        @pl.when(b > me)
        def _():
            remote(
                parts.at[b], right_sums.at[b], send_right.at[b], receive_right.at[b], me
            ).wait_send()

        @pl.when(b < me)
        def _():
            remote(
                parts.at[b], left_sums.at[b], send_left.at[b], receive_left.at[b], me
            ).wait_send()

        return carry

    lax.fori_loop(0, count, drain, 0)


def attn_reduce_kernel(count, qkv_grad, out_grad, out, parts, loads, *rest):
    dps, _, piece, _ = qkv_grad.shape
    part = out_grad.shape[-1] // dps
    moves = [
        pltpu.make_async_copy(
            qkv_grad.at[i, :, :, pl.ds(g * part, part)],
            parts.at[:, pl.ds(g * piece, piece), pl.ds(i * part, part)],
            loads.at[g * dps + i],
        )
        for g in range(3)
        for i in range(dps)
    ]
    moves.append(
        pltpu.make_async_copy(
            out_grad, parts.at[:, pl.ds(3 * piece, piece), :], loads.at[3 * dps]
        )
    )
    for move in moves:
        move.start()
    for move in moves:
        move.wait()
    reduce_kernel(count, parts, out, *rest)


def reduce_attn(qkv_grad, out_grad, number):
    count = lax.axis_size("expert")
    dps = lax.axis_size("dp")
    width = out_grad.shape[1]
    piece = out_grad.shape[0] // count
    qkv_grad = qkv_grad.reshape(dps, count, piece, qkv_grad.shape[1])
    out_grad = out_grad.reshape(count, piece, width)
    shape = (count, 4 * piece, width)
    return pl.pallas_call(
        functools.partial(attn_reduce_kernel, count),
        out_shape=jax.ShapeDtypeStruct(shape[1:], jnp.float32),
        in_specs=[pl.BlockSpec(memory_space=pl.ANY)] * 2,
        out_specs=pl.BlockSpec(memory_space=pltpu.VMEM),
        scratch_shapes=[
            pltpu.VMEM(shape, out_grad.dtype),
            pltpu.SemaphoreType.DMA((3 * dps + 1,)),
        ]
        + [pltpu.VMEM(shape, out_grad.dtype)] * 2
        + [pltpu.SemaphoreType.DMA((count,))] * 4,
        compiler_params=pltpu.CompilerParams(
            collective_id=number, has_side_effects=True, vmem_limit_bytes=LIMIT
        ),
        cost_estimate=pl.CostEstimate(
            flops=0, bytes_accessed=30 * math.prod(shape), transcendentals=0
        ),
    )(qkv_grad, out_grad)


def reduce_rows(parts, number):
    count = lax.axis_size("expert")
    parts = parts.reshape(count, -1, parts.shape[-1])
    return pl.pallas_call(
        functools.partial(reduce_kernel, count),
        out_shape=jax.ShapeDtypeStruct(parts.shape[1:], jnp.float32),
        in_specs=[pl.BlockSpec(memory_space=pltpu.VMEM)],
        out_specs=pl.BlockSpec(memory_space=pltpu.VMEM),
        scratch_shapes=[pltpu.VMEM(parts.shape, parts.dtype)] * 2
        + [pltpu.SemaphoreType.DMA((count,))] * 4,
        compiler_params=pltpu.CompilerParams(
            collective_id=number, has_side_effects=True, vmem_limit_bytes=LIMIT
        ),
        cost_estimate=pl.CostEstimate(
            flops=0, bytes_accessed=30 * parts.size, transcendentals=0
        ),
    )(parts)


def sum_small(values, devices):
    flat = jnp.concatenate([v.reshape(-1) for v in values])
    size = flat.shape[0]
    chunk = -(-size // (devices * 128)) * 128
    flat = jnp.pad(flat, (0, devices * chunk - size)).reshape(devices, chunk)
    flat = swap(flat, BOTH)
    total = spread(jnp.sum(flat, axis=0), BOTH, devices).reshape(-1)
    out, at = [], 0
    for v in values:
        out.append(total[at : at + v.size].reshape(v.shape))
        at += v.size
    return out


def on_device(
    tokens,
    teacher,
    qkv_weight,
    out_weight,
    query_gain,
    key_gain,
    attn_gain,
    ffn_gain,
    router_weight,
    gate_up_weight,
    down_weight,
    deal,
    routes,
    counted,
    lengths,
):
    bf16 = jnp.bfloat16
    f32 = jnp.float32
    rows, width = tokens.shape
    slots = routes.shape[1]
    experts = router_weight.shape[1]
    local = gate_up_weight.shape[0]
    hidden = gate_up_weight.shape[2] // 2
    owners = lax.axis_size("expert")
    dps = lax.axis_size("dp")
    devices = dps * owners
    stripe = rows // devices
    my_dp = lax.axis_index("dp")
    my_ex = lax.axis_index("expert")
    part = width // dps
    piece = part // owners
    heads = part // HD
    group = dps * rows
    factor = HD ** (-0.5)

    lanes = 128
    packed = jnp.concatenate(
        [
            routes.reshape(-1),
            counted,
            jnp.pad(lengths[0], (0, lanes - lengths.shape[1])),
        ]
    )
    packed = spread(packed, BOTH, devices)
    packed = packed.reshape(dps, owners, -1)
    total_count = jnp.sum(packed[:, :, rows * slots : rows * slots + rows]).astype(f32)
    valid_total = jnp.maximum(total_count, 1.0)
    group_routes = lax.dynamic_index_in_dim(packed, my_dp, 0, keepdims=False)
    group_routes = group_routes[:, : rows * slots].reshape(owners * rows, slots)
    group_lengths = lax.dynamic_index_in_dim(packed, my_ex, 1, keepdims=False)
    group_lengths = group_lengths[:, rows * slots + rows :][:, : lengths.shape[1]]

    dealt_tokens = swap(tokens.reshape(devices, stripe, width)[deal], BOTH)
    dealt_tokens = dealt_tokens.reshape(rows, width)
    dealt_teacher = swap(teacher.reshape(devices, stripe, width)[deal], BOTH).reshape(rows, width)

    gate_up = []
    for e in range(local):
        gate_up.append(lax.all_gather(gate_up_weight[e], "dp", axis=0, tiled=True))
    down = lax.all_gather(down_weight, "dp", axis=1, tiled=True)
    down = down.reshape(local * hidden, width)

    ends = jnp.cumsum(group_lengths, axis=1)
    index = jnp.arange(rows, dtype=jnp.int32)
    passed = (index[None, :, None] >= ends[:, None, :]).astype(jnp.int32)
    segment = jnp.sum(passed, axis=2)
    start = jnp.sum(passed * group_lengths[:, None, :], axis=2)
    inverse = jnp.exp(
        jnp.arange(HD // 2, dtype=f32) * (-2.0 * math.log(ROPE_BASE) / HD)
    )
    angles = (index[None, :] - start).astype(f32)[:, :, None] * inverse
    cosine = jnp.cos(angles)[:, :, None, :]
    sine_part = jnp.sin(angles)[:, :, None, :]
    same = (segment[:, :, None] == segment[:, None, :])[:, None]

    mine = lax.dynamic_slice_in_dim(qkv_weight, my_ex * piece, piece, axis=0)
    mine = jnp.stack(
        [
            jnp.concatenate(
                [mine[:, g * width + d * part : g * width + (d + 1) * part] for g in range(3)],
                axis=1,
            )
            for d in range(dps)
        ]
    )
    mine = swap(mine, "dp").reshape(dps * piece, 3 * part)
    weight_cols = gather_rows(mine, 1)
    weight_cols = weight_cols.reshape(owners, dps, piece, 3 * part).transpose(1, 0, 2, 3)
    weight_cols = weight_cols.reshape(width, 3 * part)
    tokens32 = dealt_tokens.astype(f32)
    attn_scale = rms_scale(tokens32)
    attn_normed = tokens32 * attn_scale
    attn_low = (attn_normed * attn_gain).astype(bf16)
    attn_rows = spread(attn_low, "dp", dps).reshape(group, width)
    qkv = dotf(attn_rows, weight_cols, ((1,), (0,)))
    queries, keys, values_low = (
        qkv[:, g * part : (g + 1) * part].reshape(dps, rows, heads, HD) for g in range(3)
    )
    values_low = values_low.astype(bf16)
    query_scale = rms_scale(queries)
    query_normed = queries * query_scale
    query_low = rotate(query_normed * query_gain, cosine, sine_part).astype(bf16)
    key_scale = rms_scale(keys)
    key_normed = keys * key_scale
    key_low = rotate(key_normed * key_gain, cosine, sine_part).astype(bf16)
    scores = (
        jnp.einsum("bthd,bshd->bhts", query_low, key_low, preferred_element_type=f32) * factor
    )
    scores = jnp.where(same, scores, -1e30)
    row_max = jnp.max(scores, axis=-1, keepdims=True)
    weights = jnp.exp(scores - row_max)
    probs = weights / jnp.sum(weights, axis=-1, keepdims=True)
    probs_low = probs.astype(bf16)
    mixed = jnp.einsum("bhts,bshd->bthd", probs_low, values_low, preferred_element_type=f32)
    mixed_low = mixed.reshape(group, part).astype(bf16)
    attn_out = dotf(mixed_low, out_weight, ((1,), (0,)))
    attn_out = swap(attn_out.astype(bf16).reshape(dps, rows, width), "dp")
    residual = tokens32 + jnp.sum(attn_out.astype(f32), axis=0)

    ffn_scale = rms_scale(residual)
    ffn_normed = residual * ffn_scale
    feed_low = (ffn_normed * ffn_gain).astype(bf16)
    feed = gather_rows(feed_low, 2)
    logits = dotf(feed, router_weight, ((1,), (0,)))
    table = group_routes[:, :, None] == jnp.arange(experts, dtype=jnp.int32)
    named = jnp.any(table, axis=1)
    masked = jnp.where(named, logits, -jnp.inf)
    gates = jnp.exp(masked - jnp.max(masked, axis=1, keepdims=True))
    gates = gates / jnp.sum(gates, axis=1, keepdims=True)
    own_gates = lax.dynamic_slice_in_dim(gates, my_ex * local, local, axis=1)
    my_gates = lax.dynamic_slice_in_dim(gates, my_ex * rows, rows, axis=0)
    gate_rows, up_rows, inner = [], [], []
    for e in range(local):
        gu = dotf(feed, gate_up[e], ((1,), (0,))).astype(bf16)
        g, u = gu[:, :hidden].astype(f32), gu[:, hidden:].astype(f32)
        gate_rows.append(g)
        up_rows.append(u)
        inner.append((jax.nn.silu(g) * u * own_gates[:, e : e + 1]).astype(bf16))
    inner = jnp.concatenate(inner, axis=1)
    moe = dotf(inner, down, ((1,), (0,)))
    moe = reduce_rows(moe.astype(bf16), 3)
    result = residual + moe

    keep = counted.astype(f32)[:, None]
    error_rows = result - dealt_teacher.astype(f32)
    part_square = jnp.sum(keep * error_rows * error_rows)
    grad_result = (2.0 * (rows * devices) / valid_total) * keep * error_rows

    grad_rows = gather_rows(grad_result.astype(bf16), 4)
    output_rows, grad_rows = lax.optimization_barrier((result.astype(bf16), grad_rows))
    back_output = swap(output_rows.reshape(devices, stripe, width), BOTH)
    grad_feed = 0.0
    gate_grads, grad_gus = [], []
    grad_inner_raw = dotf(grad_rows, down, ((1,), (1,))).astype(bf16)
    for e in range(local):
        g, u = gate_rows[e], up_rows[e]
        sg = jax.nn.sigmoid(g)
        silu = g * sg
        raw = grad_inner_raw[:, e * hidden : (e + 1) * hidden].astype(f32)
        gate_grads.append(jnp.sum(raw * (silu * u), axis=1))
        grad_inner = raw * own_gates[:, e : e + 1]
        grad_g = grad_inner * u * sg * (1.0 + g * (1.0 - sg))
        grad_u = grad_inner * silu
        grad_gu = jnp.concatenate([grad_g, grad_u], axis=1).astype(bf16)
        grad_gus.append(grad_gu)
        grad_feed = grad_feed + dotf(grad_gu, gate_up[e], ((1,), (1,)))
    grad_down_w = dotf(inner, grad_rows, ((0,), (0,))).astype(bf16)
    grad_feed = reduce_rows(grad_feed.astype(bf16), 5)
    grad_gate_up_w = []
    for e in range(local):
        grad_gate_up_w.append(dotf(feed, grad_gus[e], ((0,), (0,))).astype(bf16))
    gate_grad = swap(
        jnp.stack(gate_grads, axis=0).reshape(local, owners, rows).transpose(1, 0, 2), "expert"
    )
    gate_grad = gate_grad.reshape(experts, rows).T
    grad_logits = my_gates * (gate_grad - jnp.sum(my_gates * gate_grad, axis=1, keepdims=True))
    grad_router = lax.dot_general(
        feed_low.astype(f32),
        grad_logits,
        (((0,), (0,)), ((), ())),
        precision=lax.Precision.HIGHEST,
        preferred_element_type=f32,
    )
    grad_feed = grad_feed + lax.dot_general(
        grad_logits,
        router_weight.astype(f32),
        (((1,), (1,)), ((), ())),
        precision=lax.Precision.HIGHEST,
        preferred_element_type=f32,
    )
    grad_ffn_gain = jnp.sum(grad_feed * ffn_normed, axis=0)
    grad_resid = grad_result + norm_back(grad_feed * ffn_gain, ffn_normed, ffn_scale)

    grad_attn = spread(grad_resid.astype(bf16), "dp", dps)
    grad_attn = grad_attn.reshape(group, width)
    grad_out_w = dotf(mixed_low, grad_attn, ((0,), (0,))).astype(bf16)
    grad_mixed = dotf(grad_attn, out_weight, ((1,), (1,)))
    grad_mixed = grad_mixed.reshape(dps, rows, heads, HD).astype(bf16)
    grad_probs = jnp.einsum("bthd,bshd->bhts", grad_mixed, values_low, preferred_element_type=f32)
    weighted = jnp.sum(probs * grad_probs, axis=-1, keepdims=True)
    grad_scores = (probs * (grad_probs - weighted)).astype(bf16)
    grad_value = jnp.einsum("bhts,bthd->bshd", probs_low, grad_mixed, preferred_element_type=f32)
    grad_query = (
        jnp.einsum("bhts,bshd->bthd", grad_scores, key_low, preferred_element_type=f32) * factor
    )
    grad_key = (
        jnp.einsum("bhts,bthd->bshd", grad_scores, query_low, preferred_element_type=f32) * factor
    )
    grad_qn = rotate(grad_query, cosine, -sine_part)
    grad_query_gain = jnp.sum(grad_qn * query_normed, axis=(0, 1, 2))
    grad_q = norm_back(grad_qn * query_gain, query_normed, query_scale)
    grad_kn = rotate(grad_key, cosine, -sine_part)
    grad_key_gain = jnp.sum(grad_kn * key_normed, axis=(0, 1, 2))
    grad_k = norm_back(grad_kn * key_gain, key_normed, key_scale)
    grad_qkv = jnp.concatenate(
        [
            grad_q.reshape(group, part).astype(bf16),
            grad_k.reshape(group, part).astype(bf16),
            grad_value.reshape(group, part).astype(bf16),
        ],
        axis=1,
    )
    grad_normed = dotf(grad_qkv, weight_cols, ((1,), (1,)))
    grad_attn_gain = jnp.sum(grad_normed * attn_rows.astype(f32), axis=0) / attn_gain
    grad_normed = grad_normed.astype(bf16)
    grad_normed = swap(grad_normed.reshape(dps, rows, width), "dp")
    grad_normed = jnp.sum(grad_normed.astype(f32), axis=0)
    grad_qkv_w = dotf(attn_rows, grad_qkv, ((0,), (0,))).astype(bf16)
    grad_tokens = grad_resid + norm_back(grad_normed * attn_gain, attn_normed, attn_scale)

    attn_grads = reduce_attn(grad_qkv_w, grad_out_w, 6)
    out_out = attn_grads[3 * piece :]
    grad_qkv_w = attn_grads[: 3 * piece].astype(bf16).reshape(3 * piece, dps, part)
    grad_qkv_w = swap(grad_qkv_w.transpose(1, 0, 2), "dp")
    qkv_out = jnp.concatenate(
        [grad_qkv_w[d, g * piece : (g + 1) * piece] for g in range(3) for d in range(dps)], axis=1
    ).astype(f32)
    down_out = lax.psum_scatter(
        grad_down_w.reshape(local, hidden, width), "dp", scatter_dimension=1, tiled=True
    )
    down_out = down_out.astype(f32)
    gate_up_out = []
    for e in range(local):
        gate_up_out.append(
            lax.psum_scatter(grad_gate_up_w[e], "dp", scatter_dimension=0, tiled=True)
        )
    gate_up_out = jnp.stack([w.astype(f32) for w in gate_up_out])
    sums = sum_small(
        (part_square, grad_query_gain, grad_key_gain, grad_attn_gain, grad_ffn_gain, grad_router),
        devices,
    )
    mean_loss = sums[0] / (valid_total * width)

    inverse_deal = (
        jnp.zeros((devices,), jnp.int32).at[deal].set(jnp.arange(devices, dtype=jnp.int32))
    )
    back_grad = swap(grad_tokens.astype(bf16).reshape(devices, stripe, width), BOTH)
    output = back_output[inverse_deal].reshape(rows, width)
    given_grad = back_grad[inverse_deal].reshape(rows, width).astype(f32)
    return (
        output,
        mean_loss,
        given_grad,
        qkv_out,
        out_out,
        sums[1],
        sums[2],
        sums[3],
        sums[4],
        sums[5],
        gate_up_out,
        down_out,
    )


def solution(mesh):
    placed = (
        P(BOTH, None),
        P(BOTH, None),
        P("dp", None),
        P("dp", None),
        P(),
        P(),
        P(),
        P(),
        P(),
        P("expert", "dp", None),
        P("expert", "dp", None),
        P(),
        P(BOTH, None),
        P(BOTH),
        P(BOTH, None),
    )
    return jax.shard_map(
        on_device,
        mesh=mesh,
        in_specs=placed,
        out_specs=(
            P(BOTH, None),
            P(),
            P(BOTH, None),
            P(BOTH, None),
            P(BOTH, None),
            P(),
            P(),
            P(),
            P(),
            P(),
            P("expert", "dp", None),
            P("expert", "dp", None),
        ),
        check_vma=False,
    )
```

```python
import functools
import math

import jax
import jax.numpy as jnp
from jax import lax
from jax.experimental import pallas as pl
from jax.experimental.pallas import tpu as pltpu
from jax.sharding import PartitionSpec as P

HD = 128
EPS = 1e-06
ROPE_BASE = 50000.0
BOTH = ("dp", "expert")
LIMIT = 60 * 1024 * 1024


def rms_scale(values):
    return lax.rsqrt(jnp.mean(values * values, axis=-1, keepdims=True) + EPS)


def rotate(values, cosine, sine_part):
    half = values.shape[-1] // 2
    a, b = values[..., :half], values[..., half:]
    return jnp.concatenate([a * cosine - b * sine_part, b * cosine + a * sine_part], axis=-1)


def norm_back(grad_in, normed, scale_rows):
    return scale_rows * (grad_in - normed * jnp.mean(grad_in * normed, axis=-1, keepdims=True))


def dotf(left, right, dims):
    return lax.dot_general(left, right, (dims, ((), ())), preferred_element_type=jnp.float32)


def swap(pieces, axes):
    return lax.all_to_all(pieces, axes, split_axis=0, concat_axis=0, tiled=True)


def spread(block, axes, count):
    return swap(jnp.broadcast_to(block[None], (count, *block.shape)), axes)


def neighbour(index):
    return {"expert": index}


def meet_neighbours(me, count):
    barrier = pltpu.get_barrier_semaphore()

    @pl.when(me > 0)
    def _():
        pl.semaphore_signal(
            barrier, inc=1, device_id=neighbour(me - 1), device_id_type=pl.DeviceIdType.MESH
        )

    @pl.when(me < count - 1)
    def _():
        pl.semaphore_signal(
            barrier, inc=1, device_id=neighbour(me + 1), device_id_type=pl.DeviceIdType.MESH
        )

    ends = ((me == 0) | (me == count - 1)).astype(jnp.int32)
    pl.semaphore_wait(barrier, 2 - ends)


def remote(source, target, send, receive, index):
    return pltpu.make_async_remote_copy(
        src_ref=source,
        dst_ref=target,
        send_sem=send,
        recv_sem=receive,
        device_id=neighbour(index),
        device_id_type=pl.DeviceIdType.MESH,
    )


def gather_kernel(count, block, out, send_right, send_left, receive):
    me = lax.axis_index("expert")
    meet_neighbours(me, count)

    @pl.when(me < count - 1)
    def _():
        remote(block, out.at[me], send_right.at[me], receive.at[me], me + 1).start()

    @pl.when(me > 0)
    def _():
        remote(block, out.at[me], send_left.at[me], receive.at[me], me - 1).start()

    out[me] = block[...]

    def step(s, carry):
        low, high = me - s, me + s

        @pl.when(low >= 0)
        def _():
            remote(out.at[low], out.at[low], send_right.at[low], receive.at[low], me).wait_recv()

            @pl.when(me < count - 1)
            def _():
                remote(
                    out.at[low], out.at[low], send_right.at[low], receive.at[low], me + 1
                ).start()

        @pl.when(high < count)
        def _():
            remote(out.at[high], out.at[high], send_left.at[high], receive.at[high], me).wait_recv()

            @pl.when(me > 0)
            def _():
                remote(
                    out.at[high], out.at[high], send_left.at[high], receive.at[high], me - 1
                ).start()

        return carry

    lax.fori_loop(1, count, step, 0)

    def drain(b, carry):
        @pl.when((b <= me) & (me < count - 1))
        def _():
            remote(block, out.at[b], send_right.at[b], receive.at[b], me + 1).wait_send()

        @pl.when((b >= me) & (me > 0))
        def _():
            remote(block, out.at[b], send_left.at[b], receive.at[b], me - 1).wait_send()

        return carry

    lax.fori_loop(0, count, drain, 0)


def gather_rows(block, number):
    count = lax.axis_size("expert")
    out = pl.pallas_call(
        functools.partial(gather_kernel, count),
        out_shape=jax.ShapeDtypeStruct((count, *block.shape), block.dtype),
        in_specs=[pl.BlockSpec(memory_space=pltpu.VMEM)],
        out_specs=pl.BlockSpec(memory_space=pltpu.VMEM),
        scratch_shapes=[pltpu.SemaphoreType.DMA((count,))] * 3,
        compiler_params=pltpu.CompilerParams(
            collective_id=number, has_side_effects=True, vmem_limit_bytes=LIMIT
        ),
        cost_estimate=pl.CostEstimate(
            flops=0, bytes_accessed=30 * count * block.size, transcendentals=0
        ),
    )(block)
    return out.reshape(count * block.shape[0], *block.shape[1:])


def add_rows(left, right, out):
    rows = out.shape[0]
    step = 16

    def body(r, carry):
        at = pl.ds(pl.multiple_of(r * step, step), step)
        out[at] = (left[at].astype(jnp.float32) + right[at].astype(jnp.float32)).astype(out.dtype)
        return carry

    lax.fori_loop(0, rows // step, body, 0)


def reduce_kernel(
    count, parts, out, right_sums, left_sums, send_right, send_left, receive_right, receive_left
):
    me = lax.axis_index("expert")
    meet_neighbours(me, count)

    def step(t, carry):
        high = count - 1 - (t - me)

        @pl.when((t >= me) & (high > me))
        def _():
            @pl.when(me == 0)
            def _():
                remote(
                    parts.at[high],
                    right_sums.at[high],
                    send_right.at[high],
                    receive_right.at[high],
                    me + 1,
                ).start()

            @pl.when(me > 0)
            def _():
                move = remote(
                    right_sums.at[high],
                    right_sums.at[high],
                    send_right.at[high],
                    receive_right.at[high],
                    me + 1,
                )
                move.wait_recv()
                add_rows(right_sums.at[high], parts.at[high], right_sums.at[high])
                move.start()

        low = t - (count - 1 - me)

        @pl.when((low >= 0) & (low < me))
        def _():
            @pl.when(me == count - 1)
            def _():
                remote(
                    parts.at[low],
                    left_sums.at[low],
                    send_left.at[low],
                    receive_left.at[low],
                    me - 1,
                ).start()

            @pl.when(me < count - 1)
            def _():
                move = remote(
                    left_sums.at[low],
                    left_sums.at[low],
                    send_left.at[low],
                    receive_left.at[low],
                    me - 1,
                )
                move.wait_recv()
                add_rows(left_sums.at[low], parts.at[low], left_sums.at[low])
                move.start()

        return carry

    lax.fori_loop(0, count - 1, step, 0)

    @pl.when(me == 0)
    def _():
        remote(
            left_sums.at[me], left_sums.at[me], send_left.at[me], receive_left.at[me], me
        ).wait_recv()
        add_rows(parts.at[me], left_sums.at[me], out)

    @pl.when(me > 0)
    def _():
        remote(
            right_sums.at[me], right_sums.at[me], send_right.at[me], receive_right.at[me], me
        ).wait_recv()
        add_rows(parts.at[me], right_sums.at[me], out)

        @pl.when(me < count - 1)
        def _():
            remote(
                left_sums.at[me], left_sums.at[me], send_left.at[me], receive_left.at[me], me
            ).wait_recv()
            add_rows(out, left_sums.at[me], out)

    def drain(b, carry):
        @pl.when(b > me)
        def _():
            remote(
                parts.at[b], right_sums.at[b], send_right.at[b], receive_right.at[b], me
            ).wait_send()

        @pl.when(b < me)
        def _():
            remote(
                parts.at[b], left_sums.at[b], send_left.at[b], receive_left.at[b], me
            ).wait_send()

        return carry

    lax.fori_loop(0, count, drain, 0)


def attn_reduce_kernel(count, qkv_grad, out_grad, out, parts, loads, *rest):
    dps, _, piece, _ = qkv_grad.shape
    part = out_grad.shape[-1] // dps
    moves = [
        pltpu.make_async_copy(
            qkv_grad.at[i, :, :, pl.ds(g * part, part)],
            parts.at[:, pl.ds(g * piece, piece), pl.ds(i * part, part)],
            loads.at[g * dps + i],
        )
        for g in range(3)
        for i in range(dps)
    ]
    moves.append(
        pltpu.make_async_copy(
            out_grad, parts.at[:, pl.ds(3 * piece, piece), :], loads.at[3 * dps]
        )
    )
    for move in moves:
        move.start()
    for move in moves:
        move.wait()
    reduce_kernel(count, parts, out, *rest)


def reduce_attn(qkv_grad, out_grad, number):
    count = lax.axis_size("expert")
    dps = lax.axis_size("dp")
    width = out_grad.shape[1]
    piece = out_grad.shape[0] // count
    qkv_grad = qkv_grad.reshape(dps, count, piece, qkv_grad.shape[1])
    out_grad = out_grad.reshape(count, piece, width)
    shape = (count, 4 * piece, width)
    return pl.pallas_call(
        functools.partial(attn_reduce_kernel, count),
        out_shape=jax.ShapeDtypeStruct(shape[1:], jnp.float32),
        in_specs=[pl.BlockSpec(memory_space=pl.ANY)] * 2,
        out_specs=pl.BlockSpec(memory_space=pltpu.VMEM),
        scratch_shapes=[
            pltpu.VMEM(shape, out_grad.dtype),
            pltpu.SemaphoreType.DMA((3 * dps + 1,)),
        ]
        + [pltpu.VMEM(shape, out_grad.dtype)] * 2
        + [pltpu.SemaphoreType.DMA((count,))] * 4,
        compiler_params=pltpu.CompilerParams(
            collective_id=number, has_side_effects=True, vmem_limit_bytes=LIMIT
        ),
        cost_estimate=pl.CostEstimate(
            flops=0, bytes_accessed=30 * math.prod(shape), transcendentals=0
        ),
    )(qkv_grad, out_grad)


def reduce_rows(parts, number):
    count = lax.axis_size("expert")
    parts = parts.reshape(count, -1, parts.shape[-1])
    return pl.pallas_call(
        functools.partial(reduce_kernel, count),
        out_shape=jax.ShapeDtypeStruct(parts.shape[1:], jnp.float32),
        in_specs=[pl.BlockSpec(memory_space=pltpu.VMEM)],
        out_specs=pl.BlockSpec(memory_space=pltpu.VMEM),
        scratch_shapes=[pltpu.VMEM(parts.shape, parts.dtype)] * 2
        + [pltpu.SemaphoreType.DMA((count,))] * 4,
        compiler_params=pltpu.CompilerParams(
            collective_id=number, has_side_effects=True, vmem_limit_bytes=LIMIT
        ),
        cost_estimate=pl.CostEstimate(
            flops=0, bytes_accessed=30 * parts.size, transcendentals=0
        ),
    )(parts)


def sum_small(values, devices):
    flat = jnp.concatenate([v.reshape(-1) for v in values])
    size = flat.shape[0]
    chunk = -(-size // (devices * 128)) * 128
    flat = jnp.pad(flat, (0, devices * chunk - size)).reshape(devices, chunk // 128, 128)
    flat = swap(flat, BOTH)
    total = spread(jnp.sum(flat, axis=0), BOTH, devices).reshape(-1)
    out, at = [], 0
    for v in values:
        out.append(total[at : at + v.size].reshape(v.shape))
        at += v.size
    return out


def on_device(
    tokens,
    teacher,
    qkv_weight,
    out_weight,
    query_gain,
    key_gain,
    attn_gain,
    ffn_gain,
    router_weight,
    gate_up_weight,
    down_weight,
    deal,
    routes,
    counted,
    lengths,
):
    bf16 = jnp.bfloat16
    f32 = jnp.float32
    rows, width = tokens.shape
    slots = routes.shape[1]
    experts = router_weight.shape[1]
    local = gate_up_weight.shape[0]
    hidden = gate_up_weight.shape[2] // 2
    owners = lax.axis_size("expert")
    dps = lax.axis_size("dp")
    devices = dps * owners
    stripe = rows // devices
    my_dp = lax.axis_index("dp")
    my_ex = lax.axis_index("expert")
    part = width // dps
    piece = part // owners
    heads = part // HD
    group = dps * rows
    factor = HD ** (-0.5)

    lanes = 128
    packed = jnp.concatenate(
        [
            routes.reshape(-1),
            counted,
            jnp.pad(lengths[0], (0, lanes - lengths.shape[1])),
        ]
    )
    packed = spread(packed.reshape(-1, lanes), BOTH, devices)
    packed = packed.reshape(dps, owners, -1)
    total_count = jnp.sum(packed[:, :, rows * slots : rows * slots + rows]).astype(f32)
    valid_total = jnp.maximum(total_count, 1.0)
    group_routes = lax.dynamic_index_in_dim(packed, my_dp, 0, keepdims=False)
    group_routes = group_routes[:, : rows * slots].reshape(owners * rows, slots)
    group_lengths = lax.dynamic_index_in_dim(packed, my_ex, 1, keepdims=False)
    group_lengths = group_lengths[:, rows * slots + rows :][:, : lengths.shape[1]]

    dealt_tokens = swap(tokens.reshape(devices, stripe, width)[deal], BOTH)
    dealt_tokens = dealt_tokens.reshape(rows, width)
    dealt_teacher = swap(teacher.reshape(devices, stripe, width)[deal], BOTH).reshape(rows, width)

    gate_up = lax.all_gather(
        jnp.concatenate([gate_up_weight[e] for e in range(local)], axis=1),
        "dp",
        axis=0,
        tiled=True,
    )
    down = lax.all_gather(down_weight, "dp", axis=1, tiled=True)
    down = down.reshape(local * hidden, width)

    ends = jnp.cumsum(group_lengths, axis=1)
    index = jnp.arange(rows, dtype=jnp.int32)
    passed = (index[None, :, None] >= ends[:, None, :]).astype(jnp.int32)
    segment = jnp.sum(passed, axis=2)
    start = jnp.sum(passed * group_lengths[:, None, :], axis=2)
    inverse = jnp.exp(
        jnp.arange(HD // 2, dtype=f32) * (-2.0 * math.log(ROPE_BASE) / HD)
    )
    angles = (index[None, :] - start).astype(f32)[:, :, None] * inverse
    cosine = jnp.cos(angles)[:, :, None, :]
    sine_part = jnp.sin(angles)[:, :, None, :]
    same = (segment[:, :, None] == segment[:, None, :])[:, None]

    mine = lax.dynamic_slice_in_dim(qkv_weight, my_ex * piece, piece, axis=0)
    mine = jnp.stack(
        [
            jnp.concatenate(
                [mine[:, g * width + d * part : g * width + (d + 1) * part] for g in range(3)],
                axis=1,
            )
            for d in range(dps)
        ]
    )
    mine = swap(mine, "dp").reshape(dps * piece, 3 * part)
    weight_cols = gather_rows(mine, 1)
    weight_cols = weight_cols.reshape(owners, dps, piece, 3 * part).transpose(1, 0, 2, 3)
    weight_cols = weight_cols.reshape(width, 3 * part)
    tokens32 = dealt_tokens.astype(f32)
    attn_scale = rms_scale(tokens32)
    attn_normed = tokens32 * attn_scale
    attn_low = (attn_normed * attn_gain).astype(bf16)
    attn_rows = spread(attn_low, "dp", dps).reshape(group, width)
    qkv = dotf(attn_rows, weight_cols, ((1,), (0,)))
    queries, keys, values_low = (
        qkv[:, g * part : (g + 1) * part].reshape(dps, rows, heads, HD) for g in range(3)
    )
    values_low = values_low.astype(bf16)
    query_scale = rms_scale(queries)
    query_normed = queries * query_scale
    query_low = rotate(query_normed * query_gain, cosine, sine_part).astype(bf16)
    key_scale = rms_scale(keys)
    key_normed = keys * key_scale
    key_low = rotate(key_normed * key_gain, cosine, sine_part).astype(bf16)
    scores = (
        jnp.einsum("bthd,bshd->bhts", query_low, key_low, preferred_element_type=f32) * factor
    )
    scores = jnp.where(same, scores, -1e30)
    row_max = jnp.max(scores, axis=-1, keepdims=True)
    weights = jnp.exp(scores - row_max)
    probs = weights / jnp.sum(weights, axis=-1, keepdims=True)
    probs_low = probs.astype(bf16)
    mixed = jnp.einsum("bhts,bshd->bthd", probs_low, values_low, preferred_element_type=f32)
    mixed_low = mixed.reshape(group, part).astype(bf16)
    attn_out = dotf(mixed_low, out_weight, ((1,), (0,)))
    attn_out = swap(attn_out.astype(bf16).reshape(dps, rows, width), "dp")
    residual = tokens32 + jnp.sum(attn_out.astype(f32), axis=0)

    ffn_scale = rms_scale(residual)
    ffn_normed = residual * ffn_scale
    feed_low = (ffn_normed * ffn_gain).astype(bf16)
    feed = gather_rows(feed_low, 2)
    logits = dotf(feed, router_weight, ((1,), (0,)))
    table = group_routes[:, :, None] == jnp.arange(experts, dtype=jnp.int32)
    named = jnp.any(table, axis=1)
    masked = jnp.where(named, logits, -jnp.inf)
    gates = jnp.exp(masked - jnp.max(masked, axis=1, keepdims=True))
    gates = gates / jnp.sum(gates, axis=1, keepdims=True)
    own_gates = lax.dynamic_slice_in_dim(gates, my_ex * local, local, axis=1)
    my_gates = lax.dynamic_slice_in_dim(gates, my_ex * rows, rows, axis=0)
    gate_up_rows = dotf(feed, gate_up, ((1,), (0,))).astype(bf16)
    gate_rows, up_rows, inner = [], [], []
    for e in range(local):
        at = 2 * e * hidden
        g = gate_up_rows[:, at : at + hidden].astype(f32)
        u = gate_up_rows[:, at + hidden : at + 2 * hidden].astype(f32)
        gate_rows.append(g)
        up_rows.append(u)
        inner.append((jax.nn.silu(g) * u * own_gates[:, e : e + 1]).astype(bf16))
    inner = jnp.concatenate(inner, axis=1)
    moe = dotf(inner, down, ((1,), (0,)))
    moe = reduce_rows(moe.astype(bf16), 3)
    result = residual + moe

    keep = counted.astype(f32)[:, None]
    error_rows = result - dealt_teacher.astype(f32)
    part_square = jnp.sum(keep * error_rows * error_rows)
    grad_result = (2.0 * (rows * devices) / valid_total) * keep * error_rows

    grad_rows = gather_rows(grad_result.astype(bf16), 4)
    output_rows, grad_rows = lax.optimization_barrier((result.astype(bf16), grad_rows))
    back_output = swap(output_rows.reshape(devices, stripe, width), BOTH)
    gate_grads, grad_gus = [], []
    grad_inner_raw = dotf(grad_rows, down, ((1,), (1,))).astype(bf16)
    for e in range(local):
        g, u = gate_rows[e], up_rows[e]
        sg = jax.nn.sigmoid(g)
        silu = g * sg
        raw = grad_inner_raw[:, e * hidden : (e + 1) * hidden].astype(f32)
        gate_grads.append(jnp.sum(raw * (silu * u), axis=1))
        grad_inner = raw * own_gates[:, e : e + 1]
        grad_g = grad_inner * u * sg * (1.0 + g * (1.0 - sg))
        grad_u = grad_inner * silu
        grad_gus += [grad_g.astype(bf16), grad_u.astype(bf16)]
    grad_gus = jnp.concatenate(grad_gus, axis=1)
    grad_feed = dotf(grad_gus, gate_up, ((1,), (1,))).astype(bf16)
    grad_down_w = dotf(inner, grad_rows, ((0,), (0,))).astype(bf16)
    grad_gate_up_w = []
    for e in range(local):
        at = 2 * e * hidden
        grad_gate_up_w.append(
            dotf(feed, grad_gus[:, at : at + 2 * hidden], ((0,), (0,))).astype(bf16)
        )
    grad_feed, grad_gate_up_w[0] = lax.optimization_barrier((grad_feed, grad_gate_up_w[0]))
    grad_feed = reduce_rows(grad_feed, 5)
    gate_grad = swap(
        jnp.stack(gate_grads, axis=0).reshape(local, owners, rows).transpose(1, 0, 2), "expert"
    )
    gate_grad = gate_grad.reshape(experts, rows).T
    grad_logits = my_gates * (gate_grad - jnp.sum(my_gates * gate_grad, axis=1, keepdims=True))
    grad_router = lax.dot_general(
        feed_low.astype(f32),
        grad_logits,
        (((0,), (0,)), ((), ())),
        precision=lax.Precision.HIGHEST,
        preferred_element_type=f32,
    )
    grad_feed = grad_feed + lax.dot_general(
        grad_logits,
        router_weight.astype(f32),
        (((1,), (1,)), ((), ())),
        precision=lax.Precision.HIGHEST,
        preferred_element_type=f32,
    )
    grad_ffn_gain = jnp.sum(grad_feed * ffn_normed, axis=0)
    grad_resid = grad_result + norm_back(grad_feed * ffn_gain, ffn_normed, ffn_scale)

    grad_attn = spread(grad_resid.astype(bf16), "dp", dps)
    grad_attn = grad_attn.reshape(group, width)
    grad_out_w = dotf(mixed_low, grad_attn, ((0,), (0,))).astype(bf16)
    grad_mixed = dotf(grad_attn, out_weight, ((1,), (1,)))
    grad_mixed = grad_mixed.reshape(dps, rows, heads, HD).astype(bf16)
    grad_probs = jnp.einsum("bthd,bshd->bhts", grad_mixed, values_low, preferred_element_type=f32)
    weighted = jnp.sum(probs * grad_probs, axis=-1, keepdims=True)
    grad_scores = (probs * (grad_probs - weighted)).astype(bf16)
    grad_value = jnp.einsum("bhts,bthd->bshd", probs_low, grad_mixed, preferred_element_type=f32)
    grad_query = (
        jnp.einsum("bhts,bshd->bthd", grad_scores, key_low, preferred_element_type=f32) * factor
    )
    grad_key = (
        jnp.einsum("bhts,bthd->bshd", grad_scores, query_low, preferred_element_type=f32) * factor
    )
    grad_qn = rotate(grad_query, cosine, -sine_part)
    grad_query_gain = jnp.sum(grad_qn * query_normed, axis=(0, 1, 2))
    grad_q = norm_back(grad_qn * query_gain, query_normed, query_scale)
    grad_kn = rotate(grad_key, cosine, -sine_part)
    grad_key_gain = jnp.sum(grad_kn * key_normed, axis=(0, 1, 2))
    grad_k = norm_back(grad_kn * key_gain, key_normed, key_scale)
    grad_qkv = jnp.concatenate(
        [
            grad_q.reshape(group, part).astype(bf16),
            grad_k.reshape(group, part).astype(bf16),
            grad_value.reshape(group, part).astype(bf16),
        ],
        axis=1,
    )
    grad_normed = dotf(grad_qkv, weight_cols, ((1,), (1,)))
    grad_attn_gain = jnp.sum(grad_normed * attn_rows.astype(f32), axis=0) / attn_gain
    grad_normed = grad_normed.astype(bf16)
    grad_normed = swap(grad_normed.reshape(dps, rows, width), "dp")
    grad_normed = jnp.sum(grad_normed.astype(f32), axis=0)
    grad_qkv_w = dotf(attn_rows, grad_qkv, ((0,), (0,))).astype(bf16)
    grad_tokens = grad_resid + norm_back(grad_normed * attn_gain, attn_normed, attn_scale)

    attn_grads = reduce_attn(grad_qkv_w, grad_out_w, 6)
    out_out = attn_grads[3 * piece :]
    grad_qkv_w = attn_grads[: 3 * piece].astype(bf16).reshape(3 * piece, dps, part)
    grad_qkv_w = swap(grad_qkv_w.transpose(1, 0, 2), "dp")
    qkv_out = jnp.concatenate(
        [grad_qkv_w[d, g * piece : (g + 1) * piece] for g in range(3) for d in range(dps)], axis=1
    ).astype(f32)
    down_out = lax.psum_scatter(
        grad_down_w.reshape(local, hidden, width), "dp", scatter_dimension=1, tiled=True
    )
    down_out = down_out.astype(f32)
    gate_up_out = []
    for e in range(local):
        gate_up_out.append(
            lax.psum_scatter(grad_gate_up_w[e], "dp", scatter_dimension=0, tiled=True)
        )
    gate_up_out = jnp.stack([w.astype(f32) for w in gate_up_out])
    sums = sum_small(
        (part_square, grad_query_gain, grad_key_gain, grad_attn_gain, grad_ffn_gain, grad_router),
        devices,
    )
    mean_loss = sums[0] / (valid_total * width)

    inverse_deal = (
        jnp.zeros((devices,), jnp.int32).at[deal].set(jnp.arange(devices, dtype=jnp.int32))
    )
    back_grad = swap(grad_tokens.astype(bf16).reshape(devices, stripe, width), BOTH)
    output = back_output[inverse_deal].reshape(rows, width)
    given_grad = back_grad[inverse_deal].reshape(rows, width).astype(f32)
    return (
        output,
        mean_loss,
        given_grad,
        qkv_out,
        out_out,
        sums[1],
        sums[2],
        sums[3],
        sums[4],
        sums[5],
        gate_up_out,
        down_out,
    )


def solution(mesh):
    placed = (
        P(BOTH, None),
        P(BOTH, None),
        P("dp", None),
        P("dp", None),
        P(),
        P(),
        P(),
        P(),
        P(),
        P("expert", "dp", None),
        P("expert", "dp", None),
        P(),
        P(BOTH, None),
        P(BOTH),
        P(BOTH, None),
    )
    return jax.shard_map(
        on_device,
        mesh=mesh,
        in_specs=placed,
        out_specs=(
            P(BOTH, None),
            P(),
            P(BOTH, None),
            P(BOTH, None),
            P(BOTH, None),
            P(),
            P(),
            P(),
            P(),
            P(),
            P("expert", "dp", None),
            P("expert", "dp", None),
        ),
        check_vma=False,
    )
```
